8 devices in a mesh: data: 1 (over z), tp: 2 (over y), ep: 4 (over x, core).
Axes of the slice: x: 2, y: 2, z: 1, core: 2. Of those that a mesh axis runs over, the one named last changes fastest.
Arguments:
- tokens: bfloat16 [1024, 1280], P(('data', 'ep', 'tp'))
- expert_ids: int32 [1024, 6], P(('data', 'ep', 'tp'))
- gate_vals: float32 [1024, 6], P(('data', 'ep', 'tp'))
- slot_ids: int32 [1024, 6], P(('data', 'ep', 'tp'))
- send_counts: int32 [8, 64], P(('data', 'ep', 'tp'))
- shared_w1: bfloat16 [1280, 1792], P(None, 'tp')
- shared_w3: bfloat16 [1280, 1792], P(None, 'tp')
- shared_w2: bfloat16 [1792, 1280], P('tp')
- expert_w1: bfloat16 [64, 1280, 896], P('ep')
- expert_w3: bfloat16 [64, 1280, 896], P('ep')
- expert_w2: bfloat16 [64, 896, 1280], P('ep')
Outputs:
- output: bfloat16 [1024, 1280], P(('data', 'ep', 'tp'))
All inputs are finite; a program needn't handle non-finite values.
Results may differ from the reference program's by a relative error of at most 0.00104.
Values are sent between devices in bfloat16 or wider.
A program may use at most 1 GiB of HBM per device.

```python
import jax
import jax.numpy as jnp
from jax import lax

EP = 4
TP = 2
TOKENS_DEV = 128
D = 1280
FS = 1792
FF = 896
EXPERTS = 64
TOP = 6
HOT = 8
CAP = 48

N_SRC = EP * TP
TOKENS = TOKENS_DEV * N_SRC


def draw_routing(route_key):
    key_hot, key_wts, key_perm = jax.random.split(route_key, 3)
    experts = jnp.arange(EXPERTS, dtype=jnp.int32)
    offset = jax.random.randint(key_hot, (), 0, EXPERTS, dtype=jnp.int32)
    is_hot = ((experts - offset) % EXPERTS) < HOT
    weights = jax.random.randint(key_wts, (N_SRC, EXPERTS), 1, 3, dtype=jnp.int32)
    cum_wts = jnp.cumsum(jnp.where(is_hot[None, :], 0, weights), axis=1)
    cold_total = TOKENS_DEV * TOP - HOT * CAP
    bounds = (cold_total * cum_wts) // cum_wts[:, -1:]
    prev_bounds = jnp.concatenate([jnp.zeros((N_SRC, 1), jnp.int32), bounds[:, :-1]], axis=1)
    counts = jnp.where(is_hot[None, :], CAP, bounds - prev_bounds).astype(jnp.int32)
    run_ends = jnp.cumsum(counts, axis=1)
    copy_pos = jnp.arange(TOKENS_DEV * TOP, dtype=jnp.int32)
    expert_of = jax.vmap(lambda end_row: jnp.searchsorted(end_row, copy_pos, side="right"))(run_ends).astype(jnp.int32)
    slot_of = copy_pos[None, :] - jnp.take_along_axis(run_ends - counts, expert_of, axis=1)
    expert_of = expert_of.reshape(N_SRC, TOP, TOKENS_DEV).transpose(0, 2, 1)
    slot_of = slot_of.reshape(N_SRC, TOP, TOKENS_DEV).transpose(0, 2, 1)
    tok_perms = jax.vmap(lambda perm_key: jax.random.permutation(perm_key, TOKENS_DEV))(jax.random.split(key_perm, N_SRC))
    expert_of = jnp.take_along_axis(expert_of, tok_perms[:, :, None], axis=1)
    slot_of = jnp.take_along_axis(slot_of, tok_perms[:, :, None], axis=1)
    return expert_of.reshape(TOKENS, TOP).astype(jnp.int32), slot_of.reshape(TOKENS, TOP).astype(jnp.int32), counts


def scaled_normal(weight_key, shape, fan_in):
    return (jax.random.normal(weight_key, shape, jnp.float32) * fan_in ** -0.5).astype(jnp.bfloat16)


def setup_inputs(seed: int = 0, part: int = 0) -> dict:
    base_key = jax.random.key(seed)
    part_key = jax.random.fold_in(base_key, part)
    key_x, key_gate, key_route = jax.random.split(part_key, 3)
    weight_keys = jax.random.split(jax.random.key(seed + 1), 6)
    tokens = jax.random.normal(key_x, (TOKENS, D), jnp.float32).astype(jnp.bfloat16)
    expert_ids, slot_ids, send_counts = draw_routing(key_route)
    gate_vals = jax.random.uniform(key_gate, (TOKENS, TOP), jnp.float32, 0.5, 1.5) * TOP ** -0.5
    return {
        "tokens": tokens,
        "expert_ids": expert_ids,
        "gate_vals": gate_vals,
        "slot_ids": slot_ids,
        "send_counts": send_counts,
        "shared_w1": scaled_normal(weight_keys[0], (D, FS), D),
        "shared_w3": scaled_normal(weight_keys[1], (D, FS), D),
        "shared_w2": scaled_normal(weight_keys[2], (FS, D), FS),
        "expert_w1": scaled_normal(weight_keys[3], (EXPERTS, D, FF), D),
        "expert_w3": scaled_normal(weight_keys[4], (EXPERTS, D, FF), D),
        "expert_w2": scaled_normal(weight_keys[5], (EXPERTS, FF, D), FF),
    }


def shared_block(tok_block, shared_w1, shared_w3, shared_w2):
    pre_gate = jnp.dot(tok_block, shared_w1, preferred_element_type=jnp.float32)
    pre_up = jnp.dot(tok_block, shared_w3, preferred_element_type=jnp.float32)
    hidden = (jax.nn.silu(pre_gate) * pre_up).astype(jnp.bfloat16)
    return jnp.dot(hidden, shared_w2, preferred_element_type=jnp.float32)


def reference(tokens, expert_ids, gate_vals, slot_ids, send_counts, shared_w1, shared_w3, shared_w2, expert_w1, expert_w3, expert_w2):
    tok_blocks = tokens.reshape(N_SRC, TOKENS_DEV, D)
    shared_out = lax.map(lambda tok_block: shared_block(tok_block, shared_w1, shared_w3, shared_w2), tok_blocks).reshape(TOKENS, D)
    src_ids = jnp.arange(TOKENS, dtype=jnp.int32) // TOKENS_DEV
    row_limit = send_counts[src_ids[:, None], expert_ids]
    kept_mask = (slot_ids >= 0) & (slot_ids < row_limit)
    n_rows = N_SRC * EXPERTS * CAP
    dest_row = jnp.where(kept_mask, (src_ids[:, None] * EXPERTS + expert_ids) * CAP + slot_ids, n_rows)
    copy_ids = jnp.arange(TOKENS * TOP, dtype=jnp.int32)
    owner_ids = jnp.full((n_rows,), TOKENS * TOP, jnp.int32).at[dest_row.reshape(-1)].set(copy_ids, mode="drop")
    owner_ids = owner_ids.reshape(N_SRC, EXPERTS, CAP).transpose(1, 0, 2).reshape(EXPERTS, N_SRC * CAP)
    flat_gates = gate_vals.reshape(-1)

    def expert_step(running, step_in):
        w_in, w_up, w_out, own_ids = step_in
        tok_of = own_ids // TOP
        expert_rows = jnp.take(tokens, tok_of, axis=0, mode="fill", fill_value=0)
        pre_gate = jnp.dot(expert_rows, w_in, preferred_element_type=jnp.float32)
        pre_up = jnp.dot(expert_rows, w_up, preferred_element_type=jnp.float32)
        hidden = (jax.nn.silu(pre_gate) * pre_up).astype(jnp.bfloat16)
        routed = jnp.dot(hidden, w_out, preferred_element_type=jnp.float32).astype(jnp.bfloat16)
        weight = jnp.take(flat_gates, own_ids, mode="fill", fill_value=0)
        running = running.at[tok_of].add(weight[:, None] * routed.astype(jnp.float32), mode="drop")
        return running, None

    routed_sum = lax.scan(expert_step, jnp.zeros((TOKENS, D), jnp.float32), (expert_w1, expert_w3, expert_w2, owner_ids))[0]
    return (tokens.astype(jnp.float32) + shared_out + routed_sum).astype(jnp.bfloat16)
```

```python
import functools

import jax
import jax.numpy as jnp
from jax import lax
from jax.experimental import pallas as pl
from jax.experimental.pallas import tpu as pltpu
from jax.sharding import PartitionSpec as P

CAP_FACTOR = 4
BF16_MAX = 3.3895313892515355e38
SLOTS = 6

X_PART, X_FAR, X_Y, X_RELAY, M_PART, M_FAR, M_RELAY, S_Y, A_PART, B_FAR, C_PART = range(11)
N_COPIES = 11


def capacity_rows(n_tok, top_k, n_exp):
    return min(n_tok, ((CAP_FACTOR * n_tok * top_k // n_exp + 7) // 8) * 8)


def chunks(n, step=256):
    return [(i, min(step, n - i)) for i in range(0, n, step)]


def dot(a, b):
    return jnp.dot(a, b, preferred_element_type=jnp.float32)


def dot_nt(a, b):
    return lax.dot_general(a, b, (((1,), (1,)), ((), ())), preferred_element_type=jnp.float32)


def kernel(cap, n_local, n_exp,
           x_hbm, idx_hbm, gate_hbm, slot_hbm, cnt_hbm,
           ws1_hbm, ws3_hbm, ws2_hbm, w1_hbm, w3_hbm, w2_hbm,
           y_ref,
           xs, xy, idx_v, gate_v, slot_v, cnt_v, ms, w13b, w2b, xr, hf, hb, gm,
           s_own, s_send, s_recv, a_send, a_recv, b_send, b_recv, c_send, c_recv,
           in_sem, w_sem, send_sem, recv_sem):
    n_tok, d_model = x_hbm.shape
    top_k = idx_hbm.shape[1]
    ff = w1_hbm.shape[2]
    n_rows = n_local * cap

    ep = lax.axis_index("ep")
    tp = lax.axis_index("tp")
    part = ep + 1 - 2 * lax.rem(ep, 2)
    far = lax.rem(ep + 2, 4)
    far_part = lax.rem(part + 2, 4)

    x_in = pltpu.make_async_copy(x_hbm, xs.at[ep], in_sem.at[0])
    small = [
        pltpu.make_async_copy(idx_hbm, idx_v, in_sem.at[1]),
        pltpu.make_async_copy(gate_hbm, gate_v, in_sem.at[2]),
        pltpu.make_async_copy(slot_hbm, slot_v, in_sem.at[3]),
        pltpu.make_async_copy(cnt_hbm, cnt_v, in_sem.at[4]),
    ]
    x_in.start()
    for cp in small:
        cp.start()

    def weight_copies(r1, r3, r2, slot):
        return [
            pltpu.make_async_copy(r1, w13b.at[slot, :, pl.ds(0, ff)], w_sem.at[slot, 0]),
            pltpu.make_async_copy(r3, w13b.at[slot, :, pl.ds(ff, ff)], w_sem.at[slot, 1]),
            pltpu.make_async_copy(r2, w2b.at[slot], w_sem.at[slot, 2]),
        ]

    def expert_copies(e, slot):
        return weight_copies(w1_hbm.at[e], w3_hbm.at[e], w2_hbm.at[e], slot)

    shared_copies = weight_copies(ws1_hbm, ws3_hbm, ws2_hbm, 0)
    for cp in shared_copies:
        cp.start()
    for e in range(SLOTS - 1):
        for cp in expert_copies(e, e + 1):
            cp.start()

    barrier = pltpu.get_barrier_semaphore()
    for dev in ({"ep": part}, {"ep": far}, {"tp": 1 - tp}):
        pl.semaphore_signal(barrier, inc=1, device_id=dev, device_id_type=pl.DeviceIdType.MESH)
    pl.semaphore_wait(barrier, 3)

    def remote(src, dst, k, dev):
        return pltpu.make_async_remote_copy(
            src_ref=src, dst_ref=dst, send_sem=send_sem.at[k], recv_sem=recv_sem.at[k],
            device_id=dev, device_id_type=pl.DeviceIdType.MESH)

    x_in.wait()
    x_far = remote(xs.at[ep], xs.at[ep], X_FAR, {"ep": far})
    x_y = remote(xs.at[ep], xy, X_Y, {"tp": 1 - tp})
    x_part = remote(xs.at[ep], xs.at[ep], X_PART, {"ep": part})
    x_far.start()
    x_y.start()
    x_part.start()

    for cp in small:
        cp.wait()
    lane = lax.broadcasted_iota(jnp.int32, (n_tok, 2 * n_exp), 1)
    low = lane < n_exp
    lane_e = jnp.where(low, lane, lane - n_exp)
    dup = jnp.where(
        lax.broadcasted_iota(jnp.int32, (n_exp, 2 * n_exp), 0)
        == jnp.where(lax.broadcasted_iota(jnp.int32, (n_exp, 2 * n_exp), 1) < n_exp,
                     lax.broadcasted_iota(jnp.int32, (n_exp, 2 * n_exp), 1),
                     lax.broadcasted_iota(jnp.int32, (n_exp, 2 * n_exp), 1) - n_exp),
        1.0, 0.0).astype(jnp.bfloat16)
    cnt = dot(jnp.broadcast_to(cnt_v[...].astype(jnp.float32), (8, n_exp)).astype(jnp.bfloat16), dup)
    limit = jnp.broadcast_to(cnt[0:1, :], (n_tok, 2 * n_exp))
    g = gate_v[...]
    g1 = jnp.minimum(g, BF16_MAX).astype(jnp.bfloat16).astype(jnp.float32)
    g2 = (g - g1).astype(jnp.bfloat16).astype(jnp.float32)
    g3 = (g - g1) - g2
    slot_f = slot_v[...].astype(jnp.float32)
    ids = idx_v[...]
    tab_a = jnp.zeros((n_tok, 2 * n_exp), jnp.float32)
    tab_b = jnp.zeros((n_tok, 2 * n_exp), jnp.float32)
    for j in range(top_k):
        s_j = slot_f[:, j:j + 1]
        kept = (ids[:, j:j + 1] == lane_e) & (s_j >= 0.0) & (s_j < limit)
        tab_a += jnp.where(kept, jnp.where(low, s_j + 1.0, g1[:, j:j + 1]), 0.0)
        tab_b += jnp.where(kept, jnp.where(low, g2[:, j:j + 1], g3[:, j:j + 1]), 0.0)
    ms[ep, :, 0:2 * n_exp] = tab_a.astype(jnp.bfloat16)
    ms[ep, :, 2 * n_exp:4 * n_exp] = tab_b.astype(jnp.bfloat16)
    m_far = remote(ms.at[ep], ms.at[ep], M_FAR, {"ep": far})
    m_part = remote(ms.at[ep], ms.at[ep], M_PART, {"ep": part})
    m_far.start()
    m_part.start()

    def row_of(shape, dim):
        flat = lax.broadcasted_iota(jnp.int32, shape, dim)
        owner = lax.shift_right_logical(flat * 683, 15)
        return flat, owner

    def gather_rows(s):
        flat, owner = row_of((n_rows, 2 * n_exp), 0)
        lanes = lax.broadcasted_iota(jnp.int32, (n_rows, 2 * n_exp), 1)
        sel = jnp.where(lanes == owner + n_local * ep, 1.0, 0.0).astype(jnp.bfloat16)
        at = dot_nt(sel, ms[s, :, 0:2 * n_exp])
        flat, owner = row_of((n_rows, n_tok), 0)
        want = (flat - owner * cap + 1).astype(jnp.float32)
        pick = jnp.where(at == want, 1.0, 0.0).astype(jnp.bfloat16)
        for c, w in chunks(d_model):
            xr[s, :, c:c + w] = dot(pick, xs[s, :, c:c + w]).astype(jnp.bfloat16)

    def build_gates(s):
        lanes = lax.broadcasted_iota(jnp.int32, (2 * n_exp, n_rows), 0)
        _, owner = row_of((2 * n_exp, n_rows), 1)
        sel_lo = jnp.where(lanes == owner + n_local * ep, 1.0, 0.0).astype(jnp.bfloat16)
        sel_hi = jnp.where(lanes == owner + n_local * ep + n_exp, 1.0, 0.0).astype(jnp.bfloat16)
        flat, owner = row_of((n_tok, n_rows), 1)
        want = (flat - owner * cap + 1).astype(jnp.float32)
        a = ms[s, :, 0:2 * n_exp]
        b = ms[s, :, 2 * n_exp:4 * n_exp]
        hit = dot(a, sel_lo) == want
        gm[s, 0] = jnp.where(hit, dot(a, sel_hi), 0.0).astype(jnp.bfloat16)
        gm[s, 1] = jnp.where(hit, dot(b, sel_lo), 0.0).astype(jnp.bfloat16)
        gm[s, 2] = jnp.where(hit, dot(b, sel_hi), 0.0).astype(jnp.bfloat16)

    def hidden(rows, x_val, slot):
        for c, w in chunks(2 * ff):
            hf[0:rows, c:c + w] = dot(x_val, w13b[slot, :, c:c + w])
        for c, w in chunks(ff):
            a = hf[0:rows, c:c + w]
            b = hf[0:rows, ff + c:ff + c + w]
            hb[0:rows, c:c + w] = (jax.nn.silu(a) * b).astype(jnp.bfloat16)

    gather_rows(ep)
    build_gates(ep)
    x_part.wait_recv()
    m_part.wait_recv()
    gather_rows(part)
    build_gates(part)

    x_far.wait_recv()
    x_relay = remote(xs.at[far], xs.at[far], X_RELAY, {"ep": part})
    x_relay.start()
    m_far.wait_recv()
    m_relay = remote(ms.at[far], ms.at[far], M_RELAY, {"ep": part})
    m_relay.start()

    x_y.wait_recv()
    for cp in shared_copies:
        cp.wait()
    hidden(2 * n_tok, jnp.concatenate([xs[ep], xy[...]], axis=0), 0)
    for c, w in chunks(d_model):
        both = dot(hb[0:2 * n_tok, :], w2b[0, :, c:c + w])
        s_own[:, c:c + w] = both[0:n_tok]
        s_send[:, c:c + w] = both[n_tok:2 * n_tok]
    s_copy = remote(s_send, s_recv, S_Y, {"tp": 1 - tp})
    s_copy.start()
    for cp in expert_copies(SLOTS - 1, 0):
        cp.start()

    gather_rows(far)
    build_gates(far)
    x_relay.wait_recv()
    m_relay.wait_recv()
    gather_rows(far_part)
    build_gates(far_part)

    n_src = xs.shape[0]

    def expert_step(e, carry):
        slot = lax.rem(e + 1, SLOTS)
        for cp in expert_copies(e, slot):
            cp.wait()
        rows = pl.ds(pl.multiple_of(e * cap, 16), cap)
        x_val = jnp.concatenate([xr[s, rows, :] for s in range(n_src)], axis=0)
        hidden(n_src * cap, x_val, slot)
        for c, w in chunks(d_model):
            out = dot(hb[0:n_src * cap, :], w2b[slot, :, c:c + w]).astype(jnp.bfloat16)
            for s in range(n_src):
                xr[s, rows, c:c + w] = out[s * cap:(s + 1) * cap]

        @pl.when(e + SLOTS < n_local)
        def _():
            for cp in expert_copies(e + SLOTS, slot):
                cp.start()

        return carry

    lax.fori_loop(0, n_local, expert_step, 0)

    def combine(s, out_ref):
        for c, w in chunks(d_model):
            r = xr[s, :, c:c + w]
            out_ref[:, c:c + w] = dot(gm[s, 0], r) + dot(gm[s, 1], r) + dot(gm[s, 2], r)

    combine(far_part, a_send)
    a_copy = remote(a_send, a_recv, A_PART, {"ep": part})
    a_copy.start()
    combine(far, b_send)
    a_copy.wait_recv()
    b_send[...] += a_recv[...]
    b_copy = remote(b_send, b_recv, B_FAR, {"ep": far})
    b_copy.start()
    combine(part, c_send)
    c_copy = remote(c_send, c_recv, C_PART, {"ep": part})
    c_copy.start()
    for c, w in chunks(d_model):
        r = xr[ep, :, c:c + w]
        own = dot(gm[ep, 0], r) + dot(gm[ep, 1], r) + dot(gm[ep, 2], r)
        s_own[:, c:c + w] += own + xs[ep, :, c:c + w].astype(jnp.float32)
    s_copy.wait_recv()
    c_copy.wait_recv()
    s_own[...] += s_recv[...] + c_recv[...]
    b_copy.wait_recv()
    y_ref[...] = (s_own[...] + b_recv[...]).astype(jnp.bfloat16)

    for cp in (x_far, x_y, x_part, m_far, m_part, x_relay, m_relay, s_copy, a_copy, b_copy, c_copy):
        cp.wait_send()


def solution(mesh):
    row_spec = P(("data", "ep", "tp"), None)
    expert_spec = P("ep", None, None)
    n_src = mesh.shape["ep"]

    def layer_body(tokens, expert_ids, gate_vals, slot_ids, send_counts, shared_w1, shared_w3, shared_w2, expert_w1, expert_w3, expert_w2):
        n_tok, d_model = tokens.shape
        top_k = expert_ids.shape[1]
        n_local, _, ff = expert_w1.shape
        n_exp = n_local * n_src
        cap = capacity_rows(n_tok, top_k, n_exp)
        n_rows = n_local * cap
        block = pltpu.VMEM((n_tok, d_model), jnp.float32)
        return pl.pallas_call(
            functools.partial(kernel, cap, n_local, n_exp),
            out_shape=jax.ShapeDtypeStruct((n_tok, d_model), jnp.bfloat16),
            in_specs=[pl.BlockSpec(memory_space=pl.ANY)] * 11,
            out_specs=pl.BlockSpec(memory_space=pltpu.VMEM),
            scratch_shapes=[
                pltpu.VMEM((n_src, n_tok, d_model), jnp.bfloat16),
                pltpu.VMEM((n_tok, d_model), jnp.bfloat16),
                pltpu.VMEM((n_tok, top_k), jnp.int32),
                pltpu.VMEM((n_tok, top_k), jnp.float32),
                pltpu.VMEM((n_tok, top_k), jnp.int32),
                pltpu.VMEM((1, n_exp), jnp.int32),
                pltpu.VMEM((n_src, n_tok, 4 * n_exp), jnp.bfloat16),
                pltpu.VMEM((SLOTS, d_model, 2 * ff), jnp.bfloat16),
                pltpu.VMEM((SLOTS, ff, d_model), jnp.bfloat16),
                pltpu.VMEM((n_src, n_rows, d_model), jnp.bfloat16),
                pltpu.VMEM((2 * n_tok, 2 * ff), jnp.float32),
                pltpu.VMEM((2 * n_tok, ff), jnp.bfloat16),
                pltpu.VMEM((n_src, 3, n_tok, n_rows), jnp.bfloat16),
            ] + [block] * 9 + [
                pltpu.SemaphoreType.DMA((5,)),
                pltpu.SemaphoreType.DMA((SLOTS, 3)),
                pltpu.SemaphoreType.DMA((N_COPIES,)),
                pltpu.SemaphoreType.DMA((N_COPIES,)),
            ],
            compiler_params=pltpu.CompilerParams(
                collective_id=0, has_side_effects=True, vmem_limit_bytes=67043328),
            name="moe_layer",
        )(tokens, expert_ids, gate_vals, slot_ids, send_counts, shared_w1, shared_w3, shared_w2, expert_w1, expert_w3, expert_w2)

    return jax.shard_map(
        layer_body,
        mesh=mesh,
        in_specs=(row_spec, row_spec, row_spec, row_spec, row_spec, P(None, "tp"), P(None, "tp"), P("tp", None), expert_spec, expert_spec, expert_spec),
        out_specs=row_spec,
        check_vma=False,
    )
```

```python
import functools

import jax
import jax.numpy as jnp
from jax import lax
from jax.experimental import pallas as pl
from jax.experimental.pallas import tpu as pltpu
from jax.sharding import PartitionSpec as P

CAP_FACTOR = 4
BF16_MAX = 3.3895313892515355e38
SLOTS = 6

X_PART, X_FAR, X_Y, X_RELAY, M_PART, M_FAR, M_DIAG, S_Y, C_PART = range(9)
N_COPIES = 9


def capacity_rows(n_tok, top_k, n_exp):
    return min(n_tok, ((CAP_FACTOR * n_tok * top_k // n_exp + 7) // 8) * 8)


def chunks(n, step=256):
    return [(i, min(step, n - i)) for i in range(0, n, step)]


def dot(a, b):
    return jnp.dot(a, b, preferred_element_type=jnp.float32)


def dot_nt(a, b):
    return lax.dot_general(a, b, (((1,), (1,)), ((), ())), preferred_element_type=jnp.float32)


def kernel(cap, n_local, split,
           x_hbm, idx_hbm, gate_hbm, slot_hbm, cnt_hbm,
           ws1_hbm, ws3_hbm, ws2_hbm, w1_hbm, w3_hbm, w2_hbm,
           y_ref,
           xs, xy, idx_v, gate_v, slot_v, cnt_v, mt, mr, w13b, w2b, xr, hf, hb, gm_a, gm_b,
           s_own, s_send, s_recv, a_send, a_recv, b_send, b_recv, c_send, c_recv,
           in_sem, w_sem, send_sem, recv_sem, col_send, col_recv):
    n_tok, d_model = x_hbm.shape
    top_k = idx_hbm.shape[0]
    ff = w1_hbm.shape[2]
    n_src = xs.shape[0]
    n_exp = n_src * n_local
    n_rows = n_local * cap
    cols = chunks(d_model)

    ep = lax.axis_index("ep")
    tp = lax.axis_index("tp")
    part = ep + 1 - 2 * lax.rem(ep, 2)
    far = lax.rem(ep + 2, 4)
    far_part = lax.rem(part + 2, 4)

    x_in = pltpu.make_async_copy(x_hbm, xs.at[ep], in_sem.at[0])
    small = [
        pltpu.make_async_copy(idx_hbm, idx_v, in_sem.at[1]),
        pltpu.make_async_copy(gate_hbm, gate_v, in_sem.at[2]),
        pltpu.make_async_copy(slot_hbm, slot_v, in_sem.at[3]),
        pltpu.make_async_copy(cnt_hbm, cnt_v, in_sem.at[4]),
    ]
    x_in.start()
    for cp in small:
        cp.start()

    def weight_copies(r1, r3, r2, slot):
        return [
            pltpu.make_async_copy(r1, w13b.at[slot, :, pl.ds(0, ff)], w_sem.at[slot, 0]),
            pltpu.make_async_copy(r3, w13b.at[slot, :, pl.ds(ff, ff)], w_sem.at[slot, 1]),
            pltpu.make_async_copy(r2, w2b.at[slot], w_sem.at[slot, 2]),
        ]

    def expert_copies(e, slot):
        return weight_copies(w1_hbm.at[e], w3_hbm.at[e], w2_hbm.at[e], slot)

    shared_copies = weight_copies(ws1_hbm, ws3_hbm, ws2_hbm, 0)

    barrier = pltpu.get_barrier_semaphore()
    for dev in ({"ep": part}, {"ep": far}, {"ep": far_part}, {"tp": 1 - tp}):
        pl.semaphore_signal(barrier, inc=1, device_id=dev, device_id_type=pl.DeviceIdType.MESH)
    pl.semaphore_wait(barrier, 4)

    def remote(src, dst, send, recv, dev):
        return pltpu.make_async_remote_copy(
            src_ref=src, dst_ref=dst, send_sem=send, recv_sem=recv,
            device_id=dev, device_id_type=pl.DeviceIdType.MESH)

    def one_copy(src, dst, k, dev):
        return remote(src, dst, send_sem.at[k], recv_sem.at[k], dev)

    x_in.wait()
    x_far = one_copy(xs.at[ep], xs.at[ep], X_FAR, {"ep": far})
    x_y = one_copy(xs.at[ep], xy, X_Y, {"tp": 1 - tp})
    x_part = one_copy(xs.at[ep], xs.at[ep], X_PART, {"ep": part})
    x_far.start()
    x_y.start()
    x_part.start()
    for cp in shared_copies:
        cp.start()

    for cp in small:
        cp.wait()
    eye = (lax.broadcasted_iota(jnp.int32, (n_exp, n_exp), 0)
           == lax.broadcasted_iota(jnp.int32, (n_exp, n_exp), 1))
    diag = jnp.where(eye, jnp.broadcast_to(cnt_v[...], (n_exp, n_exp)).astype(jnp.float32), 0.0)
    limit = dot(diag.astype(jnp.bfloat16), jnp.ones((n_exp, n_tok), jnp.bfloat16))
    g = gate_v[...]
    g1 = jnp.minimum(g, BF16_MAX).astype(jnp.bfloat16).astype(jnp.float32)
    g2 = (g - g1).astype(jnp.bfloat16).astype(jnp.float32)
    g3 = (g - g1) - g2
    slot_f = slot_v[...].astype(jnp.float32)
    ids = idx_v[...]
    row_e = lax.broadcasted_iota(jnp.int32, (n_exp, n_tok), 0)
    tabs = [jnp.zeros((n_exp, n_tok), jnp.float32) for _ in range(4)]
    for j in range(top_k):
        s_j = slot_f[j:j + 1, :]
        kept = (ids[j:j + 1, :] == row_e) & (s_j >= 0.0) & (s_j < limit)
        vals = (s_j + 1.0, g1[j:j + 1, :], g2[j:j + 1, :], g3[j:j + 1, :])
        tabs = [t + jnp.where(kept, v, 0.0) for t, v in zip(tabs, vals)]
    for q in range(n_src):
        for k in range(4):
            mt[q, k * n_local:(k + 1) * n_local, :] = (
                tabs[k][q * n_local:(q + 1) * n_local].astype(jnp.bfloat16))
    m_far = one_copy(mt.at[far], mr.at[ep], M_FAR, {"ep": far})
    m_part = one_copy(mt.at[part], mr.at[ep], M_PART, {"ep": part})
    m_diag = one_copy(mt.at[far_part], mr.at[ep], M_DIAG, {"ep": far_part})
    m_part.start()
    m_far.start()
    m_diag.start()
    mr[ep] = mt[ep]

    for e in range(SLOTS - 1):
        for cp in expert_copies(e, e + 1):
            cp.start()

    def row_of(shape, dim, lo=0):
        flat = lax.broadcasted_iota(jnp.int32, shape, dim) + lo
        owner = lax.shift_right_logical(flat * 683, 15)
        return flat, owner

    def gather_rows(s):
        _, owner = row_of((n_rows, 4 * n_local), 0)
        lanes = lax.broadcasted_iota(jnp.int32, (n_rows, 4 * n_local), 1)
        sel = jnp.where(lanes == owner, 1.0, 0.0).astype(jnp.bfloat16)
        at = dot(sel, mr[s])
        flat, owner = row_of((n_rows, n_tok), 0)
        want = (flat - owner * cap + 1).astype(jnp.float32)
        pick = jnp.where(at == want, 1.0, 0.0).astype(jnp.bfloat16)
        for c, w in cols:
            xr[s, :, c:c + w] = dot(pick, xs[s, :, c:c + w]).astype(jnp.bfloat16)

    def build_gates(s):
        tab = jnp.transpose(mr[s].astype(jnp.float32)).astype(jnp.bfloat16)
        for ref, lo, n in ((gm_a, 0, split * cap), (gm_b, split * cap, n_rows - split * cap)):
            lanes = lax.broadcasted_iota(jnp.int32, (4 * n_local, n), 0)
            _, owner = row_of((4 * n_local, n), 1, lo)
            flat, own_t = row_of((n_tok, n), 1, lo)
            want = (flat - own_t * cap + 1).astype(jnp.float32)
            at = [dot(tab, jnp.where(lanes == owner + k * n_local, 1.0, 0.0).astype(jnp.bfloat16))
                  for k in range(4)]
            hit = at[0] == want
            for k in range(3):
                ref[s, k] = jnp.where(hit, at[k + 1], 0.0).astype(jnp.bfloat16)

    def hidden(rows, x_val, slot):
        for c, w in chunks(2 * ff):
            hf[0:rows, c:c + w] = dot(x_val, w13b[slot, :, c:c + w])
        for c, w in chunks(ff):
            a = hf[0:rows, c:c + w]
            b = hf[0:rows, ff + c:ff + c + w]
            hb[0:rows, c:c + w] = (jax.nn.silu(a) * b).astype(jnp.bfloat16)

    def shared(x_val, out_ref):
        hidden(n_tok, x_val, 0)
        for c, w in cols:
            out_ref[:, c:c + w] = dot(hb[0:n_tok, :], w2b[0, :, c:c + w])

    gather_rows(ep)
    build_gates(ep)
    for cp in shared_copies:
        cp.wait()
    shared(xs[ep], s_own)
    x_part.wait_recv()
    m_part.wait_recv()
    gather_rows(part)
    build_gates(part)

    x_far.wait_recv()
    x_relay = one_copy(xs.at[far], xs.at[far], X_RELAY, {"ep": part})
    x_relay.start()
    x_y.wait_recv()
    shared(xy[...], s_send)
    s_copy = one_copy(s_send, s_recv, S_Y, {"tp": 1 - tp})
    s_copy.start()
    for cp in expert_copies(SLOTS - 1, 0):
        cp.start()

    m_far.wait_recv()
    gather_rows(far)
    build_gates(far)
    x_relay.wait_recv()
    m_diag.wait_recv()
    gather_rows(far_part)
    build_gates(far_part)

    def expert_step(e, carry):
        slot = lax.rem(e + 1, SLOTS)
        for cp in expert_copies(e, slot):
            cp.wait()
        rows = pl.ds(pl.multiple_of(e * cap, 16), cap)
        x_val = jnp.concatenate([xr[s, rows, :] for s in range(n_src)], axis=0)
        hidden(n_src * cap, x_val, slot)
        for c, w in cols:
            out = dot(hb[0:n_src * cap, :], w2b[slot, :, c:c + w]).astype(jnp.bfloat16)
            for s in range(n_src):
                xr[s, rows, c:c + w] = out[s * cap:(s + 1) * cap]

        @pl.when(e + SLOTS < n_local)
        def _():
            for cp in expert_copies(e + SLOTS, slot):
                cp.start()

        return carry

    def combine(gm, s, lo, hi, c, w):
        r = xr[s, lo:hi, c:c + w]
        return dot(gm[s, 0], r) + dot(gm[s, 1], r) + dot(gm[s, 2], r)

    cut = split * cap
    lax.fori_loop(0, split, expert_step, 0)
    for c, w in cols:
        a_send[:, c:c + w] = combine(gm_a, far_part, 0, cut, c, w)
        b_send[:, c:c + w] = combine(gm_a, far, 0, cut, c, w)
        c_send[:, c:c + w] = combine(gm_a, part, 0, cut, c, w)
        s_own[:, c:c + w] += combine(gm_a, ep, 0, cut, c, w) + xs[ep, :, c:c + w].astype(jnp.float32)
    lax.fori_loop(split, n_local, expert_step, 0)

    def col_copy(src, dst, kind, i, dev):
        c, w = cols[i]
        return remote(src.at[:, pl.ds(c, w)], dst.at[:, pl.ds(c, w)],
                      col_send.at[kind, i], col_recv.at[kind, i], dev)

    a_copies = [col_copy(a_send, a_recv, 0, i, {"ep": part}) for i in range(len(cols))]
    b_copies = [col_copy(b_send, b_recv, 1, i, {"ep": far}) for i in range(len(cols))]
    for i, (c, w) in enumerate(cols):
        a_send[:, c:c + w] += combine(gm_b, far_part, cut, n_rows, c, w)
        a_copies[i].start()
    for i, (c, w) in enumerate(cols):
        b_part = b_send[:, c:c + w] + combine(gm_b, far, cut, n_rows, c, w)
        a_copies[i].wait_recv()
        b_send[:, c:c + w] = b_part + a_recv[:, c:c + w]
        b_copies[i].start()
    for c, w in cols:
        c_send[:, c:c + w] += combine(gm_b, part, cut, n_rows, c, w)
    c_copy = one_copy(c_send, c_recv, C_PART, {"ep": part})
    c_copy.start()
    for c, w in cols:
        s_own[:, c:c + w] += combine(gm_b, ep, cut, n_rows, c, w)
    s_copy.wait_recv()
    c_copy.wait_recv()
    s_own[...] += s_recv[...] + c_recv[...]
    for i, (c, w) in enumerate(cols):
        b_copies[i].wait_recv()
        y_ref[:, c:c + w] = (s_own[:, c:c + w] + b_recv[:, c:c + w]).astype(jnp.bfloat16)

    for cp in [x_far, x_y, x_part, m_far, m_part, m_diag, x_relay, s_copy, c_copy] + a_copies + b_copies:
        cp.wait_send()


def solution(mesh):
    row_spec = P(("data", "ep", "tp"), None)
    expert_spec = P("ep", None, None)
    n_src = mesh.shape["ep"]

    def layer_body(tokens, expert_ids, gate_vals, slot_ids, send_counts, shared_w1, shared_w3, shared_w2, expert_w1, expert_w3, expert_w2):
        n_tok, d_model = tokens.shape
        top_k = expert_ids.shape[1]
        n_local, _, ff = expert_w1.shape
        n_exp = n_local * n_src
        cap = capacity_rows(n_tok, top_k, n_exp)
        n_rows = n_local * cap
        split = n_local * 11 // 16
        n_cols = len(chunks(d_model))
        block = pltpu.VMEM((n_tok, d_model), jnp.float32)
        return pl.pallas_call(
            functools.partial(kernel, cap, n_local, split),
            out_shape=pltpu.VMEM((n_tok, d_model), jnp.bfloat16),
            in_specs=[pl.BlockSpec(memory_space=pl.ANY)] * 11,
            out_specs=pl.BlockSpec(memory_space=pltpu.VMEM),
            scratch_shapes=[
                pltpu.VMEM((n_src, n_tok, d_model), jnp.bfloat16),
                pltpu.VMEM((n_tok, d_model), jnp.bfloat16),
                pltpu.VMEM((top_k, n_tok), jnp.int32),
                pltpu.VMEM((top_k, n_tok), jnp.float32),
                pltpu.VMEM((top_k, n_tok), jnp.int32),
                pltpu.VMEM((1, n_exp), jnp.int32),
                pltpu.VMEM((n_src, 4 * n_local, n_tok), jnp.bfloat16),
                pltpu.VMEM((n_src, 4 * n_local, n_tok), jnp.bfloat16),
                pltpu.VMEM((SLOTS, d_model, 2 * ff), jnp.bfloat16),
                pltpu.VMEM((SLOTS, ff, d_model), jnp.bfloat16),
                pltpu.VMEM((n_src, n_rows, d_model), jnp.bfloat16),
                pltpu.VMEM((2 * n_tok, 2 * ff), jnp.float32),
                pltpu.VMEM((2 * n_tok, ff), jnp.bfloat16),
                pltpu.VMEM((n_src, 3, n_tok, split * cap), jnp.bfloat16),
                pltpu.VMEM((n_src, 3, n_tok, n_rows - split * cap), jnp.bfloat16),
            ] + [block] * 9 + [
                pltpu.SemaphoreType.DMA((5,)),
                pltpu.SemaphoreType.DMA((SLOTS, 3)),
                pltpu.SemaphoreType.DMA((N_COPIES,)),
                pltpu.SemaphoreType.DMA((N_COPIES,)),
                pltpu.SemaphoreType.DMA((2, n_cols)),
                pltpu.SemaphoreType.DMA((2, n_cols)),
            ],
            compiler_params=pltpu.CompilerParams(
                collective_id=0, has_side_effects=True, vmem_limit_bytes=66500000),
            name="moe_layer",
        )(tokens, expert_ids.T, gate_vals.T, slot_ids.T, send_counts, shared_w1, shared_w3, shared_w2, expert_w1, expert_w3, expert_w2)

    return jax.shard_map(
        layer_body,
        mesh=mesh,
        in_specs=(row_spec, row_spec, row_spec, row_spec, row_spec, P(None, "tp"), P(None, "tp"), P("tp", None), expert_spec, expert_spec, expert_spec),
        out_specs=row_spec,
        check_vma=False,
    )
```

```python
import functools

import jax
import jax.numpy as jnp
from jax import lax
from jax.experimental import pallas as pl
from jax.experimental.pallas import tpu as pltpu
from jax.sharding import PartitionSpec as P

CAP_FACTOR = 4
BF16_MAX = 3.3895313892515355e38
SLOTS = 6
NEAR = 2

X_PART, X_Y, M_PART, M_FAR, M_DIAG, S_Y, C_PART = range(7)
N_COPIES = 7
COL_X_FAR, COL_X_RELAY, COL_A, COL_B = range(4)
N_COL_KINDS = 4


def capacity_rows(n_tok, top_k, n_exp):
    return min(n_tok, ((CAP_FACTOR * n_tok * top_k // n_exp + 7) // 8) * 8)


def chunks(n, step=256):
    return [(i, min(step, n - i)) for i in range(0, n, step)]


def dot(a, b):
    return jnp.dot(a, b, preferred_element_type=jnp.float32)


def dot_nt(a, b):
    return lax.dot_general(a, b, (((1,), (1,)), ((), ())), preferred_element_type=jnp.float32)


def kernel(cap, n_local,
           x_hbm, idx_hbm, gate_hbm, slot_hbm, cnt_hbm,
           ws1_hbm, ws3_hbm, ws2_hbm, w1_hbm, w3_hbm, w2_hbm,
           y_ref,
           xs, xy, idx_v, gate_v, slot_v, cnt_v, mt, mr, w13b, w2b, xr, hb, pk, gm,
           s_own, s_send, s_recv, a_send, a_recv, b_send, b_recv, c_send, c_recv,
           in_sem, w_sem, send_sem, recv_sem, col_send, col_recv):
    n_tok, d_model = x_hbm.shape
    top_k = idx_hbm.shape[0]
    ff = w1_hbm.shape[2]
    body = ff // 256 * 256
    rest = ff - body
    n_src = xs.shape[0]
    n_exp = n_src * n_local
    n_rows = n_local * cap
    cols = chunks(d_model)

    ep = lax.axis_index("ep")
    tp = lax.axis_index("tp")
    part = ep + 1 - 2 * lax.rem(ep, 2)
    far = lax.rem(ep + 2, 4)
    far_part = lax.rem(part + 2, 4)

    x_in = pltpu.make_async_copy(x_hbm, xs.at[ep], in_sem.at[0])
    small = [
        pltpu.make_async_copy(idx_hbm, idx_v, in_sem.at[1]),
        pltpu.make_async_copy(gate_hbm, gate_v, in_sem.at[2]),
        pltpu.make_async_copy(slot_hbm, slot_v, in_sem.at[3]),
        pltpu.make_async_copy(cnt_hbm, cnt_v, in_sem.at[4]),
    ]
    for cp in small:
        cp.start()
    x_in.start()

    def weight_copies(r1, r3, r2, slot):
        parts = [(r1, 0, 0, body), (r3, 0, body, body),
                 (r1, body, 2 * body, rest), (r3, body, 2 * body + rest, rest)]
        return [
            pltpu.make_async_copy(r.at[:, pl.ds(src, n)], w13b.at[slot, :, pl.ds(dst, n)], w_sem.at[slot, i])
            for i, (r, src, dst, n) in enumerate(parts)
        ] + [pltpu.make_async_copy(r2, w2b.at[slot], w_sem.at[slot, 4])]

    def expert_copies(e, slot):
        return weight_copies(w1_hbm.at[e], w3_hbm.at[e], w2_hbm.at[e], slot)

    def start_all(copies):
        for cp in copies:
            cp.start()

    shared_copies = weight_copies(ws1_hbm, ws3_hbm, ws2_hbm, 0)
    start_all(shared_copies)
    start_all(expert_copies(0, 1))

    barrier = pltpu.get_barrier_semaphore()
    for dev in ({"ep": part}, {"ep": far}, {"ep": far_part}, {"tp": 1 - tp}):
        pl.semaphore_signal(barrier, inc=1, device_id=dev, device_id_type=pl.DeviceIdType.MESH)

    for cp in small:
        cp.wait()
    eye = (lax.broadcasted_iota(jnp.int32, (n_exp, n_exp), 0)
           == lax.broadcasted_iota(jnp.int32, (n_exp, n_exp), 1))
    diag = jnp.where(eye, jnp.broadcast_to(cnt_v[...], (n_exp, n_exp)).astype(jnp.float32), 0.0)
    limit = dot(diag.astype(jnp.bfloat16), jnp.ones((n_exp, n_tok), jnp.bfloat16))
    g = gate_v[...]
    g1 = jnp.minimum(g, BF16_MAX).astype(jnp.bfloat16).astype(jnp.float32)
    g2 = (g - g1).astype(jnp.bfloat16).astype(jnp.float32)
    g3 = (g - g1) - g2
    slot_f = slot_v[...].astype(jnp.float32)
    ids = idx_v[...]
    row_e = lax.broadcasted_iota(jnp.int32, (n_exp, n_tok), 0)
    tabs = [jnp.zeros((n_exp, n_tok), jnp.float32) for _ in range(4)]
    for j in range(top_k):
        s_j = slot_f[j:j + 1, :]
        kept = (ids[j:j + 1, :] == row_e) & (s_j >= 0.0) & (s_j < limit)
        vals = (s_j + 1.0, g1[j:j + 1, :], g2[j:j + 1, :], g3[j:j + 1, :])
        tabs = [t + jnp.where(kept, v, 0.0) for t, v in zip(tabs, vals)]
    for q in range(n_src):
        for k in range(4):
            mt[q, k * n_local:(k + 1) * n_local, :] = (
                tabs[k][q * n_local:(q + 1) * n_local].astype(jnp.bfloat16))
    mr[ep] = mt[ep]

    pl.semaphore_wait(barrier, 4)

    def remote(src, dst, send, recv, dev):
        return pltpu.make_async_remote_copy(
            src_ref=src, dst_ref=dst, send_sem=send, recv_sem=recv,
            device_id=dev, device_id_type=pl.DeviceIdType.MESH)

    def one_copy(src, dst, k, dev):
        return remote(src, dst, send_sem.at[k], recv_sem.at[k], dev)

    def col_copies(src, dst, kind, dev):
        return [remote(src.at[:, pl.ds(c, w)], dst.at[:, pl.ds(c, w)],
                       col_send.at[kind, i], col_recv.at[kind, i], dev)
                for i, (c, w) in enumerate(cols)]

    m_far = one_copy(mt.at[far], mr.at[ep], M_FAR, {"ep": far})
    m_part = one_copy(mt.at[part], mr.at[ep], M_PART, {"ep": part})
    m_diag = one_copy(mt.at[far_part], mr.at[ep], M_DIAG, {"ep": far_part})
    x_far = col_copies(xs.at[ep], xs.at[ep], COL_X_FAR, {"ep": far})
    x_relay = col_copies(xs.at[far], xs.at[far], COL_X_RELAY, {"ep": part})
    x_y = one_copy(xs.at[ep], xy, X_Y, {"tp": 1 - tp})
    x_part = one_copy(xs.at[ep], xs.at[ep], X_PART, {"ep": part})
    m_far.start()
    m_diag.start()
    m_part.start()
    x_in.wait()
    start_all(x_far)
    x_part.start()
    x_y.start()

    for e in range(1, SLOTS - 1):
        start_all(expert_copies(e, e + 1))

    def row_of(shape, dim):
        flat = lax.broadcasted_iota(jnp.int32, shape, dim)
        owner = lax.shift_right_logical(flat * 683, 15)
        return flat, owner

    def build_pick(s, i):
        _, owner = row_of((n_rows, 4 * n_local), 0)
        lanes = lax.broadcasted_iota(jnp.int32, (n_rows, 4 * n_local), 1)
        sel = jnp.where(lanes == owner, 1.0, 0.0).astype(jnp.bfloat16)
        at = dot(sel, mr[s])
        flat, owner = row_of((n_rows, n_tok), 0)
        want = (flat - owner * cap + 1).astype(jnp.float32)
        pk[i] = jnp.where(at == want, 1.0, 0.0).astype(jnp.bfloat16)

    def gather_cols(s, i, c, w):
        xr[s, :, c:c + w] = dot(pk[i], xs[s, :, c:c + w]).astype(jnp.bfloat16)

    def build_gates(s):
        tab = jnp.transpose(mr[s].astype(jnp.float32)).astype(jnp.bfloat16)
        lanes = lax.broadcasted_iota(jnp.int32, (4 * n_local, n_rows), 0)
        _, owner = row_of((4 * n_local, n_rows), 1)
        flat, own_t = row_of((n_tok, n_rows), 1)
        want = (flat - own_t * cap + 1).astype(jnp.float32)
        at = [dot(tab, jnp.where(lanes == owner + k * n_local, 1.0, 0.0).astype(jnp.bfloat16))
              for k in range(4)]
        hit = at[0] == want
        for k in range(3):
            gm[s, k] = jnp.where(hit, at[k + 1], 0.0).astype(jnp.bfloat16)

    def hidden(x_val, slot, h_ref):
        rows = x_val.shape[0]
        for c, w in chunks(body):
            a = dot(x_val, w13b[slot, :, c:c + w])
            b = dot(x_val, w13b[slot, :, body + c:body + c + w])
            h_ref[0:rows, c:c + w] = (jax.nn.silu(a) * b).astype(jnp.bfloat16)
        ab = dot(x_val, w13b[slot, :, 2 * body:2 * ff])
        h_ref[0:rows, body:ff] = (jax.nn.silu(ab[:, 0:rest]) * ab[:, rest:2 * rest]).astype(jnp.bfloat16)

    def shared(x_val, out_ref):
        hidden(x_val, 0, hb.at[0])
        for c, w in cols:
            out_ref[:, c:c + w] = dot(hb[0, 0:n_tok, :], w2b[0, :, c:c + w])

    def wait_expert(e, slot):
        for cp in expert_copies(e, slot):
            cp.wait()

    def expert_rows(e, slot, sources, i):
        rows = pl.ds(pl.multiple_of(e * cap, 16), cap)
        n = len(sources) * cap
        hidden(jnp.concatenate([xr[s, rows, :] for s in sources], axis=0), slot, hb.at[i])
        for c, w in cols:
            out = dot(hb[i, 0:n, :], w2b[slot, :, c:c + w]).astype(jnp.bfloat16)
            for k, s in enumerate(sources):
                xr[s, rows, c:c + w] = out[k * cap:(k + 1) * cap]

    build_pick(ep, 0)
    for c, w in cols:
        gather_cols(ep, 0, c, w)
    m_part.wait_recv()
    build_pick(part, 1)
    x_part.wait_recv()
    for c, w in cols:
        gather_cols(part, 1, c, w)
    for cp in shared_copies:
        cp.wait()
    shared(xs[ep], s_own)
    m_far.wait_recv()
    build_pick(far, 0)
    build_gates(far)
    m_diag.wait_recv()
    build_pick(far_part, 1)
    build_gates(far_part)
    for e in range(NEAR):
        wait_expert(e, e + 1)
    for e in range(NEAR):
        expert_rows(e, e + 1, (ep, part), e % 2)

    for i, (c, w) in enumerate(cols):
        x_far[i].wait_recv()
        x_relay[i].start()
        gather_cols(far, 0, c, w)
    x_y.wait_recv()
    shared(xy[...], s_send)
    s_copy = one_copy(s_send, s_recv, S_Y, {"tp": 1 - tp})
    s_copy.start()
    start_all(expert_copies(SLOTS - 1, 0))
    for i, (c, w) in enumerate(cols):
        x_relay[i].wait_recv()
        gather_cols(far_part, 1, c, w)
    for e in range(NEAR):
        expert_rows(e, e + 1, (far, far_part), e % 2)
    for e in range(NEAR):
        start_all(expert_copies(e + SLOTS, e + 1))

    def pair_step(p, carry):
        both = [(2 * p + i, lax.rem(2 * p + i + 1, SLOTS)) for i in range(2)]
        for e, slot in both:
            wait_expert(e, slot)
        for i, (e, slot) in enumerate(both):
            expert_rows(e, slot, range(n_src), i)

        @pl.when(2 * p + SLOTS < n_local)
        def _():
            for e, slot in both:
                start_all(expert_copies(e + SLOTS, slot))

        return carry

    lax.fori_loop(NEAR // 2, n_local // 2, pair_step, 0)

    def combine(s, c, w):
        r = xr[s, :, c:c + w]
        return dot(gm[s, 0], r) + dot(gm[s, 1], r) + dot(gm[s, 2], r)

    a_copies = col_copies(a_send, a_recv, COL_A, {"ep": part})
    b_copies = col_copies(b_send, b_recv, COL_B, {"ep": far})
    for i, (c, w) in enumerate(cols):
        a_send[:, c:c + w] = combine(far_part, c, w)
        a_copies[i].start()
    for i, (c, w) in enumerate(cols):
        b_part = combine(far, c, w)
        a_copies[i].wait_recv()
        b_send[:, c:c + w] = b_part + a_recv[:, c:c + w]
        b_copies[i].start()
    build_gates(part)
    for c, w in cols:
        c_send[:, c:c + w] = combine(part, c, w)
    c_copy = one_copy(c_send, c_recv, C_PART, {"ep": part})
    c_copy.start()
    build_gates(ep)
    for c, w in cols:
        s_own[:, c:c + w] += combine(ep, c, w) + xs[ep, :, c:c + w].astype(jnp.float32)
    s_copy.wait_recv()
    c_copy.wait_recv()
    s_own[...] += s_recv[...] + c_recv[...]
    for i, (c, w) in enumerate(cols):
        b_copies[i].wait_recv()
        y_ref[:, c:c + w] = (s_own[:, c:c + w] + b_recv[:, c:c + w]).astype(jnp.bfloat16)

    for cp in [x_y, x_part, m_far, m_part, m_diag, s_copy, c_copy] + x_far + x_relay + a_copies + b_copies:
        cp.wait_send()


def solution(mesh):
    row_spec = P(("data", "ep", "tp"), None)
    expert_spec = P("ep", None, None)
    n_src = mesh.shape["ep"]

    def layer_body(tokens, expert_ids, gate_vals, slot_ids, send_counts, shared_w1, shared_w3, shared_w2, expert_w1, expert_w3, expert_w2):
        n_tok, d_model = tokens.shape
        top_k = expert_ids.shape[1]
        n_local, _, ff = expert_w1.shape
        n_exp = n_local * n_src
        cap = capacity_rows(n_tok, top_k, n_exp)
        n_rows = n_local * cap
        n_cols = len(chunks(d_model))
        block = pltpu.VMEM((n_tok, d_model), jnp.float32)
        return pl.pallas_call(
            functools.partial(kernel, cap, n_local),
            out_shape=pltpu.VMEM((n_tok, d_model), jnp.bfloat16),
            in_specs=[pl.BlockSpec(memory_space=pl.ANY)] * 11,
            out_specs=pl.BlockSpec(memory_space=pltpu.VMEM),
            scratch_shapes=[
                pltpu.VMEM((n_src, n_tok, d_model), jnp.bfloat16),
                pltpu.VMEM((n_tok, d_model), jnp.bfloat16),
                pltpu.VMEM((top_k, n_tok), jnp.int32),
                pltpu.VMEM((top_k, n_tok), jnp.float32),
                pltpu.VMEM((top_k, n_tok), jnp.int32),
                pltpu.VMEM((1, n_exp), jnp.int32),
                pltpu.VMEM((n_src, 4 * n_local, n_tok), jnp.bfloat16),
                pltpu.VMEM((n_src, 4 * n_local, n_tok), jnp.bfloat16),
                pltpu.VMEM((SLOTS, d_model, 2 * ff), jnp.bfloat16),
                pltpu.VMEM((SLOTS, ff, d_model), jnp.bfloat16),
                pltpu.VMEM((n_src, n_rows, d_model), jnp.bfloat16),
                pltpu.VMEM((2, n_src * cap, ff), jnp.bfloat16),
                pltpu.VMEM((2, n_rows, n_tok), jnp.bfloat16),
                pltpu.VMEM((n_src, 3, n_tok, n_rows), jnp.bfloat16),
            ] + [block] * 9 + [
                pltpu.SemaphoreType.DMA((5,)),
                pltpu.SemaphoreType.DMA((SLOTS, 5)),
                pltpu.SemaphoreType.DMA((N_COPIES,)),
                pltpu.SemaphoreType.DMA((N_COPIES,)),
                pltpu.SemaphoreType.DMA((N_COL_KINDS, n_cols)),
                pltpu.SemaphoreType.DMA((N_COL_KINDS, n_cols)),
            ],
            compiler_params=pltpu.CompilerParams(
                collective_id=0, has_side_effects=True, vmem_limit_bytes=66500000),
            name="moe_layer",
        )(tokens, expert_ids.T, gate_vals.T, slot_ids.T, send_counts, shared_w1, shared_w3, shared_w2, expert_w1, expert_w3, expert_w2)

    return jax.shard_map(
        layer_body,
        mesh=mesh,
        in_specs=(row_spec, row_spec, row_spec, row_spec, row_spec, P(None, "tp"), P(None, "tp"), P("tp", None), expert_spec, expert_spec, expert_spec),
        out_specs=row_spec,
        check_vma=False,
    )
```

```python
import functools

import jax
import jax.numpy as jnp
from jax import lax
from jax.experimental import pallas as pl
from jax.experimental.pallas import tpu as pltpu
from jax.sharding import PartitionSpec as P

CAP_FACTOR = 4
BF16_MAX = 3.3895313892515355e38
SLOTS = 6
NEAR = 2

X_PART, X_Y, M_PART, M_FAR, M_DIAG, S_Y, C_PART = range(7)
N_COPIES = 7
COL_X_FAR, COL_X_RELAY, COL_A, COL_B = range(4)
N_COL_KINDS = 4


def capacity_rows(n_tok, top_k, n_exp):
    return min(n_tok, ((CAP_FACTOR * n_tok * top_k // n_exp + 7) // 8) * 8)


def chunks(n, step=256):
    return [(i, min(step, n - i)) for i in range(0, n, step)]


def dot(a, b):
    return jnp.dot(a, b, preferred_element_type=jnp.float32)


def dot_nt(a, b):
    return lax.dot_general(a, b, (((1,), (1,)), ((), ())), preferred_element_type=jnp.float32)


def kernel(cap, n_local,
           x_hbm, idx_hbm, gate_hbm, slot_hbm, cnt_hbm,
           ws1_hbm, ws3_hbm, ws2_hbm, w1_hbm, w3_hbm, w2_hbm,
           y_ref,
           xs, xy, idx_v, gate_v, slot_v, cnt_v, mt, mr,
           s_own, s_send, s_recv, a_send, a_recv, b_send, b_recv, c_send, c_recv,
           in_sem, w_sem, send_sem, recv_sem, col_send, col_recv, w13b, w2b, xr, hb, pk, gm):
    n_tok, d_model = x_hbm.shape
    top_k = idx_hbm.shape[0]
    ff = w1_hbm.shape[2]
    body = ff // 256 * 256
    rest = ff - body
    n_src = xs.shape[0]
    n_exp = n_src * n_local
    n_rows = n_local * cap
    cols = chunks(d_model)

    ep = lax.axis_index("ep")
    tp = lax.axis_index("tp")
    part = ep + 1 - 2 * lax.rem(ep, 2)
    far = lax.rem(ep + 2, 4)
    far_part = lax.rem(part + 2, 4)

    x_in = pltpu.make_async_copy(x_hbm, xs.at[ep], in_sem.at[0])
    small = [
        pltpu.make_async_copy(idx_hbm, idx_v, in_sem.at[1]),
        pltpu.make_async_copy(gate_hbm, gate_v, in_sem.at[2]),
        pltpu.make_async_copy(slot_hbm, slot_v, in_sem.at[3]),
        pltpu.make_async_copy(cnt_hbm, cnt_v, in_sem.at[4]),
    ]
    for cp in small:
        cp.start()
    x_in.start()

    def weight_copies(r1, r3, r2, slot):
        parts = [(r1, 0, 0, body), (r3, 0, body, body),
                 (r1, body, 2 * body, rest), (r3, body, 2 * body + rest, rest)]
        return [
            pltpu.make_async_copy(r.at[:, pl.ds(src, n)], w13b.at[slot, :, pl.ds(dst, n)], w_sem.at[slot, i])
            for i, (r, src, dst, n) in enumerate(parts)
        ] + [pltpu.make_async_copy(r2, w2b.at[slot], w_sem.at[slot, 4])]

    def expert_copies(e, slot):
        return weight_copies(w1_hbm.at[e], w3_hbm.at[e], w2_hbm.at[e], slot)

    def start_all(copies):
        for cp in copies:
            cp.start()

    shared_copies = weight_copies(ws1_hbm, ws3_hbm, ws2_hbm, 0)
    start_all(shared_copies)
    start_all(expert_copies(0, 1))

    barrier = pltpu.get_barrier_semaphore()
    for dev in ({"ep": part}, {"ep": far}, {"ep": far_part}, {"tp": 1 - tp}):
        pl.semaphore_signal(barrier, inc=1, device_id=dev, device_id_type=pl.DeviceIdType.MESH)

    for cp in small:
        cp.wait()
    eye = (lax.broadcasted_iota(jnp.int32, (n_exp, n_exp), 0)
           == lax.broadcasted_iota(jnp.int32, (n_exp, n_exp), 1))
    diag = jnp.where(eye, jnp.broadcast_to(cnt_v[...], (n_exp, n_exp)).astype(jnp.float32), 0.0)
    limit = dot(diag.astype(jnp.bfloat16), jnp.ones((n_exp, n_tok), jnp.bfloat16))
    g = gate_v[...]
    g1 = jnp.minimum(g, BF16_MAX).astype(jnp.bfloat16).astype(jnp.float32)
    g2 = (g - g1).astype(jnp.bfloat16).astype(jnp.float32)
    g3 = (g - g1) - g2
    slot_f = slot_v[...].astype(jnp.float32)
    ids = idx_v[...]
    row_e = lax.broadcasted_iota(jnp.int32, (n_exp, n_tok), 0)
    tabs = [jnp.zeros((n_exp, n_tok), jnp.float32) for _ in range(4)]
    for j in range(top_k):
        s_j = slot_f[j:j + 1, :]
        kept = (ids[j:j + 1, :] == row_e) & (s_j >= 0.0) & (s_j < limit)
        vals = (s_j + 1.0, g1[j:j + 1, :], g2[j:j + 1, :], g3[j:j + 1, :])
        tabs = [t + jnp.where(kept, v, 0.0) for t, v in zip(tabs, vals)]
    for q in range(n_src):
        for k in range(4):
            mt[q, k * n_local:(k + 1) * n_local, :] = (
                tabs[k][q * n_local:(q + 1) * n_local].astype(jnp.bfloat16))
    mr[ep] = mt[ep]

    pl.semaphore_wait(barrier, 4)

    def remote(src, dst, send, recv, dev):
        return pltpu.make_async_remote_copy(
            src_ref=src, dst_ref=dst, send_sem=send, recv_sem=recv,
            device_id=dev, device_id_type=pl.DeviceIdType.MESH)

    def one_copy(src, dst, k, dev):
        return remote(src, dst, send_sem.at[k], recv_sem.at[k], dev)

    def col_copies(src, dst, kind, dev):
        return [remote(src.at[:, pl.ds(c, w)], dst.at[:, pl.ds(c, w)],
                       col_send.at[kind, i], col_recv.at[kind, i], dev)
                for i, (c, w) in enumerate(cols)]

    m_far = one_copy(mt.at[far], mr.at[ep], M_FAR, {"ep": far})
    m_part = one_copy(mt.at[part], mr.at[ep], M_PART, {"ep": part})
    m_diag = one_copy(mt.at[far_part], mr.at[ep], M_DIAG, {"ep": far_part})
    x_far = col_copies(xs.at[ep], xs.at[ep], COL_X_FAR, {"ep": far})
    x_relay = col_copies(xs.at[far], xs.at[far], COL_X_RELAY, {"ep": part})
    x_y = one_copy(xs.at[ep], xy, X_Y, {"tp": 1 - tp})
    x_part = one_copy(xs.at[ep], xs.at[ep], X_PART, {"ep": part})
    m_far.start()
    m_diag.start()
    m_part.start()
    x_in.wait()
    start_all(x_far)
    x_part.start()
    x_y.start()

    for e in range(1, SLOTS - 1):
        start_all(expert_copies(e, e + 1))

    def row_of(shape, dim):
        flat = lax.broadcasted_iota(jnp.int32, shape, dim)
        owner = lax.shift_right_logical(flat * 683, 15)
        return flat, owner

    def build_pick(s, i):
        _, owner = row_of((n_rows, 4 * n_local), 0)
        lanes = lax.broadcasted_iota(jnp.int32, (n_rows, 4 * n_local), 1)
        sel = jnp.where(lanes == owner, 1.0, 0.0).astype(jnp.bfloat16)
        at = dot(sel, mr[s])
        flat, owner = row_of((n_rows, n_tok), 0)
        want = (flat - owner * cap + 1).astype(jnp.float32)
        pk[i] = jnp.where(at == want, 1.0, 0.0).astype(jnp.bfloat16)

    def gather_cols(s, i, c, w):
        xr[s, :, c:c + w] = dot(pk[i], xs[s, :, c:c + w]).astype(jnp.bfloat16)

    def build_gates(s):
        tab = jnp.transpose(mr[s].astype(jnp.float32)).astype(jnp.bfloat16)
        lanes = lax.broadcasted_iota(jnp.int32, (4 * n_local, n_rows), 0)
        _, owner = row_of((4 * n_local, n_rows), 1)
        flat, own_t = row_of((n_tok, n_rows), 1)
        want = (flat - own_t * cap + 1).astype(jnp.float32)
        at = [dot(tab, jnp.where(lanes == owner + k * n_local, 1.0, 0.0).astype(jnp.bfloat16))
              for k in range(4)]
        hit = at[0] == want
        for k in range(3):
            gm[s, k] = jnp.where(hit, at[k + 1], 0.0).astype(jnp.bfloat16)

    def hidden(x_val, slot, h_ref):
        rows = x_val.shape[0]
        for c, w in chunks(body):
            a = dot(x_val, w13b[slot, :, c:c + w])
            b = dot(x_val, w13b[slot, :, body + c:body + c + w])
            h_ref[0:rows, c:c + w] = (jax.nn.silu(a) * b).astype(jnp.bfloat16)
        ab = dot(x_val, w13b[slot, :, 2 * body:2 * ff])
        h_ref[0:rows, body:ff] = (jax.nn.silu(ab[:, 0:rest]) * ab[:, rest:2 * rest]).astype(jnp.bfloat16)

    def shared(x_val, out_ref):
        hidden(x_val, 0, hb.at[0])
        for c, w in cols:
            out_ref[:, c:c + w] = dot(hb[0, 0:n_tok, :], w2b[0, :, c:c + w])

    def wait_expert(e, slot):
        for cp in expert_copies(e, slot):
            cp.wait()

    def expert_rows(e, slot, sources, i):
        rows = pl.ds(pl.multiple_of(e * cap, 16), cap)
        n = len(sources) * cap
        hidden(jnp.concatenate([xr[s, rows, :] for s in sources], axis=0), slot, hb.at[i])
        for c, w in cols:
            out = dot(hb[i, 0:n, :], w2b[slot, :, c:c + w]).astype(jnp.bfloat16)
            for k, s in enumerate(sources):
                xr[s, rows, c:c + w] = out[k * cap:(k + 1) * cap]

    build_pick(ep, 0)
    for c, w in cols:
        gather_cols(ep, 0, c, w)
    m_part.wait_recv()
    build_pick(part, 1)
    x_part.wait_recv()
    for c, w in cols:
        gather_cols(part, 1, c, w)
    for cp in shared_copies:
        cp.wait()
    shared(xs[ep], s_own)
    m_far.wait_recv()
    build_pick(far, 0)
    build_gates(far)
    m_diag.wait_recv()
    build_pick(far_part, 1)
    build_gates(far_part)
    for e in range(NEAR):
        wait_expert(e, e + 1)
    for e in range(NEAR):
        expert_rows(e, e + 1, (ep, part), e % 2)

    for i, (c, w) in enumerate(cols):
        x_far[i].wait_recv()
        x_relay[i].start()
        gather_cols(far, 0, c, w)
    x_y.wait_recv()
    shared(xy[...], s_send)
    s_copy = one_copy(s_send, s_recv, S_Y, {"tp": 1 - tp})
    s_copy.start()
    start_all(expert_copies(SLOTS - 1, 0))
    for i, (c, w) in enumerate(cols):
        x_relay[i].wait_recv()
        gather_cols(far_part, 1, c, w)
    for e in range(NEAR):
        expert_rows(e, e + 1, (far, far_part), e % 2)
    for e in range(NEAR):
        start_all(expert_copies(e + SLOTS, e + 1))

    def pair_step(p, carry):
        both = [(2 * p + i, lax.rem(2 * p + i + 1, SLOTS)) for i in range(2)]
        for e, slot in both:
            wait_expert(e, slot)
        for i, (e, slot) in enumerate(both):
            expert_rows(e, slot, range(n_src), i)

        @pl.when(2 * p + SLOTS < n_local)
        def _():
            for e, slot in both:
                start_all(expert_copies(e + SLOTS, slot))

        return carry

    lax.fori_loop(NEAR // 2, n_local // 2, pair_step, 0)

    def combine(s, c, w):
        r = xr[s, :, c:c + w]
        return dot(gm[s, 0], r) + dot(gm[s, 1], r) + dot(gm[s, 2], r)

    a_copies = col_copies(a_send, a_recv, COL_A, {"ep": part})
    b_copies = col_copies(b_send, b_recv, COL_B, {"ep": far})
    for i, (c, w) in enumerate(cols):
        a_send[:, c:c + w] = combine(far_part, c, w)
        a_copies[i].start()
    for i, (c, w) in enumerate(cols):
        b_part = combine(far, c, w)
        a_copies[i].wait_recv()
        b_send[:, c:c + w] = b_part + a_recv[:, c:c + w]
        b_copies[i].start()
    build_gates(part)
    for c, w in cols:
        c_send[:, c:c + w] = combine(part, c, w)
    c_copy = one_copy(c_send, c_recv, C_PART, {"ep": part})
    c_copy.start()
    build_gates(ep)
    for c, w in cols:
        s_own[:, c:c + w] += combine(ep, c, w) + xs[ep, :, c:c + w].astype(jnp.float32)
    s_copy.wait_recv()
    c_copy.wait_recv()
    s_own[...] += s_recv[...] + c_recv[...]
    for i, (c, w) in enumerate(cols):
        b_copies[i].wait_recv()
        y_ref[:, c:c + w] = (s_own[:, c:c + w] + b_recv[:, c:c + w]).astype(jnp.bfloat16)

    for cp in [x_y, x_part, m_far, m_part, m_diag, s_copy, c_copy] + x_far + x_relay + a_copies + b_copies:
        cp.wait_send()


def solution(mesh):
    row_spec = P(("data", "ep", "tp"), None)
    expert_spec = P("ep", None, None)
    n_src = mesh.shape["ep"]

    def layer_body(tokens, expert_ids, gate_vals, slot_ids, send_counts, shared_w1, shared_w3, shared_w2, expert_w1, expert_w3, expert_w2):
        n_tok, d_model = tokens.shape
        top_k = expert_ids.shape[1]
        n_local, _, ff = expert_w1.shape
        n_exp = n_local * n_src
        cap = capacity_rows(n_tok, top_k, n_exp)
        n_rows = n_local * cap
        n_cols = len(chunks(d_model))
        block = pltpu.VMEM((n_tok, d_model), jnp.float32)
        local = [
                pltpu.VMEM((SLOTS, d_model, 2 * ff), jnp.bfloat16),
                pltpu.VMEM((SLOTS, ff, d_model), jnp.bfloat16),
                pltpu.VMEM((n_src, n_rows, d_model), jnp.bfloat16),
                pltpu.VMEM((2, n_src * cap, ff), jnp.bfloat16),
                pltpu.VMEM((2, n_rows, n_tok), jnp.bfloat16),
                pltpu.VMEM((n_src, 3, n_tok, n_rows), jnp.bfloat16),
        ]

        def body(*refs):
            pl.run_scoped(functools.partial(kernel, cap, n_local, *refs), *local)

        return pl.pallas_call(
            body,
            out_shape=pltpu.VMEM((n_tok, d_model), jnp.bfloat16),
            in_specs=[pl.BlockSpec(memory_space=pl.ANY)] * 11,
            out_specs=pl.BlockSpec(memory_space=pltpu.VMEM),
            scratch_shapes=[
                pltpu.VMEM((n_src, n_tok, d_model), jnp.bfloat16),
                pltpu.VMEM((n_tok, d_model), jnp.bfloat16),
                pltpu.VMEM((top_k, n_tok), jnp.int32),
                pltpu.VMEM((top_k, n_tok), jnp.float32),
                pltpu.VMEM((top_k, n_tok), jnp.int32),
                pltpu.VMEM((1, n_exp), jnp.int32),
                pltpu.VMEM((n_src, 4 * n_local, n_tok), jnp.bfloat16),
                pltpu.VMEM((n_src, 4 * n_local, n_tok), jnp.bfloat16),
            ] + [block] * 9 + [
                pltpu.SemaphoreType.DMA((5,)),
                pltpu.SemaphoreType.DMA((SLOTS, 5)),
                pltpu.SemaphoreType.DMA((N_COPIES,)),
                pltpu.SemaphoreType.DMA((N_COPIES,)),
                pltpu.SemaphoreType.DMA((N_COL_KINDS, n_cols)),
                pltpu.SemaphoreType.DMA((N_COL_KINDS, n_cols)),
            ],
            compiler_params=pltpu.CompilerParams(
                collective_id=0, has_side_effects=True, vmem_limit_bytes=66500000),
            name="moe_layer",
        )(tokens, expert_ids.T, gate_vals.T, slot_ids.T, send_counts, shared_w1, shared_w3, shared_w2, expert_w1, expert_w3, expert_w2)

    return jax.shard_map(
        layer_body,
        mesh=mesh,
        in_specs=(row_spec, row_spec, row_spec, row_spec, row_spec, P(None, "tp"), P(None, "tp"), P("tp", None), expert_spec, expert_spec, expert_spec),
        out_specs=row_spec,
        check_vma=False,
    )
```

```python
import functools

import jax
import jax.numpy as jnp
from jax import lax
from jax.experimental import pallas as pl
from jax.experimental.pallas import tpu as pltpu
from jax.sharding import PartitionSpec as P

CAP_FACTOR = 4
BF16_MAX = 3.3895313892515355e38
SLOTS = 6
NEAR = 2
LAST = 6

X_PART, X_Y, M_PART, M_FAR, M_DIAG, S_Y, C_PART = range(7)
N_COPIES = 7
COL_X_FAR, COL_X_RELAY, COL_A, COL_B = range(4)
N_COL_KINDS = 4


def capacity_rows(n_tok, top_k, n_exp):
    return min(n_tok, ((CAP_FACTOR * n_tok * top_k // n_exp + 7) // 8) * 8)


def chunks(n, step=256):
    return [(i, min(step, n - i)) for i in range(0, n, step)]


def dot(a, b):
    return jnp.dot(a, b, preferred_element_type=jnp.float32)


def dot_nt(a, b):
    return lax.dot_general(a, b, (((1,), (1,)), ((), ())), preferred_element_type=jnp.float32)


def kernel(cap, n_local,
           x_hbm, idx_hbm, gate_hbm, slot_hbm, cnt_hbm,
           ws1_hbm, ws3_hbm, ws2_hbm, w1_hbm, w3_hbm, w2_hbm,
           y_ref,
           xs, xy, idx_v, gate_v, slot_v, cnt_v, mt, mr,
           s_own, s_send, s_recv, a_send, a_recv, b_recv,
           in_sem, w_sem, send_sem, recv_sem, col_send, col_recv, free_sem, w13b, w2b, xr, hb, pk, gm):
    n_tok, d_model = x_hbm.shape
    top_k = idx_hbm.shape[0]
    ff = w1_hbm.shape[2]
    body = ff // 256 * 256
    rest = ff - body
    n_src = xs.shape[0]
    n_exp = n_src * n_local
    n_rows = n_local * cap
    cols = chunks(d_model)

    ep = lax.axis_index("ep")
    tp = lax.axis_index("tp")
    part = ep + 1 - 2 * lax.rem(ep, 2)
    far = lax.rem(ep + 2, 4)
    far_part = lax.rem(part + 2, 4)

    x_in = pltpu.make_async_copy(x_hbm, xs.at[ep], in_sem.at[0])
    small = [
        pltpu.make_async_copy(idx_hbm, idx_v, in_sem.at[1]),
        pltpu.make_async_copy(gate_hbm, gate_v, in_sem.at[2]),
        pltpu.make_async_copy(slot_hbm, slot_v, in_sem.at[3]),
        pltpu.make_async_copy(cnt_hbm, cnt_v, in_sem.at[4]),
    ]
    for cp in small:
        cp.start()
    x_in.start()

    def weight_copies(r1, r3, r2, slot):
        return [
            pltpu.make_async_copy(r1, w13b.at[slot, :, pl.ds(0, ff)], w_sem.at[slot, 0]),
            pltpu.make_async_copy(r3, w13b.at[slot, :, pl.ds(ff, ff)], w_sem.at[slot, 1]),
            pltpu.make_async_copy(r2, w2b.at[slot], w_sem.at[slot, 2]),
        ]

    def expert_copies(e, slot):
        return weight_copies(w1_hbm.at[e], w3_hbm.at[e], w2_hbm.at[e], slot)

    def start_all(copies):
        for cp in copies:
            cp.start()

    shared_copies = weight_copies(ws1_hbm, ws3_hbm, ws2_hbm, 0)
    start_all(shared_copies)
    start_all(expert_copies(0, 1))

    barrier = pltpu.get_barrier_semaphore()
    for dev in ({"ep": part}, {"ep": far}, {"ep": far_part}, {"tp": 1 - tp}):
        pl.semaphore_signal(barrier, inc=1, device_id=dev, device_id_type=pl.DeviceIdType.MESH)

    for cp in small:
        cp.wait()
    eye = (lax.broadcasted_iota(jnp.int32, (n_exp, n_exp), 0)
           == lax.broadcasted_iota(jnp.int32, (n_exp, n_exp), 1))
    diag = jnp.where(eye, jnp.broadcast_to(cnt_v[...], (n_exp, n_exp)).astype(jnp.float32), 0.0)
    limit = dot(diag.astype(jnp.bfloat16), jnp.ones((n_exp, n_tok), jnp.bfloat16))
    g = gate_v[...]
    g1 = jnp.minimum(g, BF16_MAX).astype(jnp.bfloat16).astype(jnp.float32)
    g2 = (g - g1).astype(jnp.bfloat16).astype(jnp.float32)
    g3 = (g - g1) - g2
    slot_f = slot_v[...].astype(jnp.float32)
    ids = idx_v[...]
    row_e = lax.broadcasted_iota(jnp.int32, (n_exp, n_tok), 0)
    tabs = [jnp.zeros((n_exp, n_tok), jnp.float32) for _ in range(4)]
    for j in range(top_k):
        s_j = slot_f[j:j + 1, :]
        kept = (ids[j:j + 1, :] == row_e) & (s_j >= 0.0) & (s_j < limit)
        vals = (s_j + 1.0, g1[j:j + 1, :], g2[j:j + 1, :], g3[j:j + 1, :])
        tabs = [t + jnp.where(kept, v, 0.0) for t, v in zip(tabs, vals)]
    for q in range(n_src):
        for k in range(4):
            mt[q, k * n_local:(k + 1) * n_local, :] = (
                tabs[k][q * n_local:(q + 1) * n_local].astype(jnp.bfloat16))
    mr[ep] = mt[ep]

    pl.semaphore_wait(barrier, 4)

    def remote(src, dst, send, recv, dev):
        return pltpu.make_async_remote_copy(
            src_ref=src, dst_ref=dst, send_sem=send, recv_sem=recv,
            device_id=dev, device_id_type=pl.DeviceIdType.MESH)

    def one_copy(src, dst, k, dev):
        return remote(src, dst, send_sem.at[k], recv_sem.at[k], dev)

    def col_copies(src, dst, kind, dev):
        return [remote(src.at[:, pl.ds(c, w)], dst.at[:, pl.ds(c, w)],
                       col_send.at[kind, i], col_recv.at[kind, i], dev)
                for i, (c, w) in enumerate(cols)]

    m_far = one_copy(mt.at[far], mr.at[ep], M_FAR, {"ep": far})
    m_part = one_copy(mt.at[part], mr.at[ep], M_PART, {"ep": part})
    m_diag = one_copy(mt.at[far_part], mr.at[ep], M_DIAG, {"ep": far_part})
    x_far = col_copies(xs.at[ep], xs.at[ep], COL_X_FAR, {"ep": far})
    x_relay = col_copies(xs.at[far], xs.at[far], COL_X_RELAY, {"ep": part})
    x_y = one_copy(xs.at[ep], xy, X_Y, {"tp": 1 - tp})
    x_part = one_copy(xs.at[ep], xs.at[ep], X_PART, {"ep": part})
    m_far.start()
    m_diag.start()
    m_part.start()
    x_in.wait()
    start_all(x_far)
    x_part.start()
    x_y.start()

    for e in range(1, SLOTS - 1):
        start_all(expert_copies(e, e + 1))

    def row_of(shape, dim):
        flat = lax.broadcasted_iota(jnp.int32, shape, dim)
        owner = lax.shift_right_logical(flat * 683, 15)
        return flat, owner

    def build_pick(s, i):
        _, owner = row_of((n_rows, 4 * n_local), 0)
        lanes = lax.broadcasted_iota(jnp.int32, (n_rows, 4 * n_local), 1)
        sel = jnp.where(lanes == owner, 1.0, 0.0).astype(jnp.bfloat16)
        at = dot(sel, mr[s])
        flat, owner = row_of((n_rows, n_tok), 0)
        want = (flat - owner * cap + 1).astype(jnp.float32)
        pk[i] = jnp.where(at == want, 1.0, 0.0).astype(jnp.bfloat16)

    def gather_cols(s, i, c, w):
        xr[s, :, c:c + w] = dot(pk[i], xs[s, :, c:c + w]).astype(jnp.bfloat16)

    def build_gates(s, i):
        tab = jnp.transpose(mr[s].astype(jnp.float32)).astype(jnp.bfloat16)
        lanes = lax.broadcasted_iota(jnp.int32, (4 * n_local, n_rows), 0)
        _, owner = row_of((4 * n_local, n_rows), 1)
        flat, own_t = row_of((n_tok, n_rows), 1)
        want = (flat - own_t * cap + 1).astype(jnp.float32)
        at = [dot(tab, jnp.where(lanes == owner + k * n_local, 1.0, 0.0).astype(jnp.bfloat16))
              for k in range(4)]
        hit = at[0] == want
        for k in range(3):
            gm[i, k] = jnp.where(hit, at[k + 1], 0.0).astype(jnp.bfloat16)

    def hidden(x_val, slot, h_ref):
        rows = x_val.shape[0]
        for c, w in chunks(body):
            a = dot(x_val, w13b[slot, :, c:c + w])
            b = dot(x_val, w13b[slot, :, ff + c:ff + c + w])
            h_ref[0:rows, c:c + w] = (jax.nn.silu(a) * b).astype(jnp.bfloat16)
        ab = dot(x_val, jnp.concatenate([w13b[slot, :, body:ff], w13b[slot, :, ff + body:2 * ff]], axis=1))
        h_ref[0:rows, body:ff] = (jax.nn.silu(ab[:, 0:rest]) * ab[:, rest:2 * rest]).astype(jnp.bfloat16)

    def shared(x_val, out_ref):
        hidden(x_val, 0, hb.at[0])
        for c, w in cols:
            out_ref[:, c:c + w] = dot(hb[0, 0:n_tok, :], w2b[0, :, c:c + w])

    def wait_expert(e, slot):
        for cp in expert_copies(e, slot):
            cp.wait()

    def expert_slice(e):
        return pl.ds(pl.multiple_of(e * cap, 16), cap)

    def take_rows(e, sources):
        return jnp.concatenate([xr[s, expert_slice(e), :] for s in sources], axis=0)

    def expert_rows(e, slot, sources, i):
        rows = expert_slice(e)
        n = len(sources) * cap
        hidden(take_rows(e, sources), slot, hb.at[i])
        for c, w in cols:
            out = dot(hb[i, 0:n, :], w2b[slot, :, c:c + w]).astype(jnp.bfloat16)
            for k, s in enumerate(sources):
                xr[s, rows, c:c + w] = out[k * cap:(k + 1) * cap]

    build_pick(ep, 0)
    for c, w in cols:
        gather_cols(ep, 0, c, w)
    m_part.wait_recv()
    build_pick(part, 1)
    x_part.wait_recv()
    for c, w in cols:
        gather_cols(part, 1, c, w)
    for cp in shared_copies:
        cp.wait()
    shared(xs[ep], s_own)
    m_far.wait_recv()
    build_pick(far, 0)
    build_gates(far, 0)
    m_diag.wait_recv()
    build_pick(far_part, 1)
    build_gates(far_part, 1)
    for e in range(NEAR):
        wait_expert(e, e + 1)
    for e in range(NEAR):
        expert_rows(e, e + 1, (ep, part), e % 2)

    for i, (c, w) in enumerate(cols):
        x_far[i].wait_recv()
        x_relay[i].start()
        gather_cols(far, 0, c, w)
    x_y.wait_recv()
    shared(xy[...], s_send)
    s_copy = one_copy(s_send, s_recv, S_Y, {"tp": 1 - tp})
    s_copy.start()
    start_all(expert_copies(SLOTS - 1, 0))
    for i, (c, w) in enumerate(cols):
        x_relay[i].wait_recv()
        gather_cols(far_part, 1, c, w)
    for e in range(NEAR):
        expert_rows(e, e + 1, (far, far_part), e % 2)
    for e in range(NEAR):
        start_all(expert_copies(e + SLOTS, e + 1))

    def pair_step(p, carry):
        both = [(2 * p + i, lax.rem(2 * p + i + 1, SLOTS)) for i in range(2)]
        for e, slot in both:
            wait_expert(e, slot)
        for i, (e, slot) in enumerate(both):
            expert_rows(e, slot, range(n_src), i)

        for e, slot in both:
            @pl.when(e + SLOTS < n_local)
            def _():
                start_all(expert_copies(e + SLOTS, slot))

        return carry

    late = n_local - LAST
    lax.fori_loop(NEAR // 2, late // 2, pair_step, 0)

    def late_hidden(t, carry):
        both = [(late + 2 * t + i, lax.rem(late + 2 * t + i + 1, SLOTS)) for i in range(2)]
        for e, slot in both:
            for cp in expert_copies(e, slot)[0:2]:
                cp.wait()
        for i, (e, slot) in enumerate(both):
            hidden(take_rows(e, (far, far_part)), slot, hb.at[t, pl.ds(2 * i * cap, 2 * cap)])
        return carry

    lax.fori_loop(0, LAST // 2, late_hidden, 0)
    for e in range(late, n_local):
        expert_copies(e, (e + 1) % SLOTS)[2].wait()

    def combine(s, i, c, w):
        r = xr[s, :, c:c + w]
        return dot(gm[i, 0], r) + dot(gm[i, 1], r) + dot(gm[i, 2], r)

    a_copies = col_copies(a_send, a_recv, COL_A, {"ep": part})
    b_copies = col_copies(s_send, b_recv, COL_B, {"ep": far})
    s_copy.wait_send()

    def finish_b(i):
        c, w = cols[i]
        a_copies[i].wait_recv()
        s_send[:, c:c + w] += a_recv[:, c:c + w]
        b_copies[i].start()

    for i, (c, w) in enumerate(cols):
        for k, e in enumerate(range(late, n_local)):
            h = hb[k // 2, 2 * (k % 2) * cap:2 * (k % 2 + 1) * cap, :]
            out = dot(h, w2b[(e + 1) % SLOTS, :, c:c + w]).astype(jnp.bfloat16)
            xr[far, e * cap:(e + 1) * cap, c:c + w] = out[0:cap]
            xr[far_part, e * cap:(e + 1) * cap, c:c + w] = out[cap:2 * cap]
        a_send[:, c:c + w] = combine(far_part, 1, c, w)
        a_copies[i].start()
        s_send[:, c:c + w] = combine(far, 0, c, w)
        if i > 0:
            finish_b(i - 1)
    build_gates(part, 0)
    finish_b(len(cols) - 1)
    pl.semaphore_signal(free_sem, inc=1, device_id={"ep": part}, device_id_type=pl.DeviceIdType.MESH)
    build_gates(ep, 1)

    def late_near(t, carry):
        for i in range(2):
            e = late + 2 * t + i
            expert_rows(e, lax.rem(e + 1, SLOTS), (ep, part), i)
        return carry

    lax.fori_loop(0, LAST // 2, late_near, 0)
    for cp in a_copies:
        cp.wait_send()
    for c, w in cols:
        a_send[:, c:c + w] = combine(part, 0, c, w)
    c_copy = one_copy(a_send, a_recv, C_PART, {"ep": part})
    pl.semaphore_wait(free_sem, 1)
    c_copy.start()
    for c, w in cols:
        s_own[:, c:c + w] += combine(ep, 1, c, w) + xs[ep, :, c:c + w].astype(jnp.float32)
    s_copy.wait_recv()
    c_copy.wait_recv()
    s_own[...] += s_recv[...] + a_recv[...]
    for i, (c, w) in enumerate(cols):
        b_copies[i].wait_recv()
        y_ref[:, c:c + w] = (s_own[:, c:c + w] + b_recv[:, c:c + w]).astype(jnp.bfloat16)

    for cp in [x_y, x_part, m_far, m_part, m_diag, c_copy] + x_far + x_relay + b_copies:
        cp.wait_send()


def solution(mesh):
    row_spec = P(("data", "ep", "tp"), None)
    expert_spec = P("ep", None, None)
    n_src = mesh.shape["ep"]

    def layer_body(tokens, expert_ids, gate_vals, slot_ids, send_counts, shared_w1, shared_w3, shared_w2, expert_w1, expert_w3, expert_w2):
        n_tok, d_model = tokens.shape
        top_k = expert_ids.shape[1]
        n_local, _, ff = expert_w1.shape
        n_exp = n_local * n_src
        cap = capacity_rows(n_tok, top_k, n_exp)
        n_rows = n_local * cap
        n_cols = len(chunks(d_model))
        block = pltpu.VMEM((n_tok, d_model), jnp.float32)
        local = [
                pltpu.VMEM((SLOTS, d_model, 2 * ff), jnp.bfloat16),
                pltpu.VMEM((SLOTS, ff, d_model), jnp.bfloat16),
                pltpu.VMEM((n_src, n_rows, d_model), jnp.bfloat16),
                pltpu.VMEM((LAST // 2, n_src * cap, ff), jnp.bfloat16),
                pltpu.VMEM((2, n_rows, n_tok), jnp.bfloat16),
                pltpu.VMEM((2, 3, n_tok, n_rows), jnp.bfloat16),
        ]

        def body(*refs):
            pl.run_scoped(functools.partial(kernel, cap, n_local, *refs), *local)

        return pl.pallas_call(
            body,
            out_shape=pltpu.VMEM((n_tok, d_model), jnp.bfloat16),
            in_specs=[pl.BlockSpec(memory_space=pl.ANY)] * 11,
            out_specs=pl.BlockSpec(memory_space=pltpu.VMEM),
            scratch_shapes=[
                pltpu.VMEM((n_src, n_tok, d_model), jnp.bfloat16),
                pltpu.VMEM((n_tok, d_model), jnp.bfloat16),
                pltpu.VMEM((top_k, n_tok), jnp.int32),
                pltpu.VMEM((top_k, n_tok), jnp.float32),
                pltpu.VMEM((top_k, n_tok), jnp.int32),
                pltpu.VMEM((1, n_exp), jnp.int32),
                pltpu.VMEM((n_src, 4 * n_local, n_tok), jnp.bfloat16),
                pltpu.VMEM((n_src, 4 * n_local, n_tok), jnp.bfloat16),
            ] + [block] * 6 + [
                pltpu.SemaphoreType.DMA((5,)),
                pltpu.SemaphoreType.DMA((SLOTS, 3)),
                pltpu.SemaphoreType.DMA((N_COPIES,)),
                pltpu.SemaphoreType.DMA((N_COPIES,)),
                pltpu.SemaphoreType.DMA((N_COL_KINDS, n_cols)),
                pltpu.SemaphoreType.DMA((N_COL_KINDS, n_cols)),
                pltpu.SemaphoreType.REGULAR,
            ],
            compiler_params=pltpu.CompilerParams(
                collective_id=0, has_side_effects=True, vmem_limit_bytes=66500000),
            name="moe_layer",
        )(tokens, expert_ids.T, gate_vals.T, slot_ids.T, send_counts, shared_w1, shared_w3, shared_w2, expert_w1, expert_w3, expert_w2)

    return jax.shard_map(
        layer_body,
        mesh=mesh,
        in_specs=(row_spec, row_spec, row_spec, row_spec, row_spec, P(None, "tp"), P(None, "tp"), P("tp", None), expert_spec, expert_spec, expert_spec),
        out_specs=row_spec,
        check_vma=False,
    )
```

```python
import functools

import jax
import jax.numpy as jnp
from jax import lax
from jax.experimental import pallas as pl
from jax.experimental.pallas import tpu as pltpu
from jax.sharding import PartitionSpec as P

CAP_FACTOR = 4
BF16_MAX = 3.3895313892515355e38
RING_A = 7
RING_B = 6
NEAR = 2
LAST = 6

X_PART, X_Y, M_PART, M_FAR, M_DIAG, S_Y, C_PART = range(7)
N_COPIES = 7
COL_X_FAR, COL_X_RELAY, COL_A, COL_B = range(4)
N_COL_KINDS = 4


def capacity_rows(n_tok, top_k, n_exp):
    return min(n_tok, ((CAP_FACTOR * n_tok * top_k // n_exp + 7) // 8) * 8)


def chunks(n, step=256):
    return [(i, min(step, n - i)) for i in range(0, n, step)]


def dot(a, b):
    return jnp.dot(a, b, preferred_element_type=jnp.float32)


def dot_nt(a, b):
    return lax.dot_general(a, b, (((1,), (1,)), ((), ())), preferred_element_type=jnp.float32)


def kernel(cap, n_local,
           x_hbm, idx_hbm, gate_hbm, slot_hbm, cnt_hbm,
           ws1_hbm, ws3_hbm, ws2_hbm, w1_hbm, w3_hbm, w2_hbm,
           y_ref,
           xs, xy, idx_v, gate_v, slot_v, cnt_v, mt, mr,
           s_own, s_send, s_recv, a_send, a_recv, b_recv,
           in_sem, a_sem, b_sem, send_sem, recv_sem, col_send, col_recv, free_sem, w13b, w2b, xr, hb, pk, gm):
    n_tok, d_model = x_hbm.shape
    top_k = idx_hbm.shape[0]
    ff = w1_hbm.shape[2]
    body = ff // 256 * 256
    rest = ff - body
    n_src = xs.shape[0]
    n_exp = n_src * n_local
    n_rows = n_local * cap
    cols = chunks(d_model)

    ep = lax.axis_index("ep")
    tp = lax.axis_index("tp")
    part = ep + 1 - 2 * lax.rem(ep, 2)
    far = lax.rem(ep + 2, 4)
    far_part = lax.rem(part + 2, 4)

    x_in = pltpu.make_async_copy(x_hbm, xs.at[ep], in_sem.at[0])
    small = [
        pltpu.make_async_copy(idx_hbm, idx_v, in_sem.at[1]),
        pltpu.make_async_copy(gate_hbm, gate_v, in_sem.at[2]),
        pltpu.make_async_copy(slot_hbm, slot_v, in_sem.at[3]),
        pltpu.make_async_copy(cnt_hbm, cnt_v, in_sem.at[4]),
    ]
    for cp in small:
        cp.start()
    x_in.start()

    def copies_a(r1, r3, step):
        at = lax.rem(step, RING_A)
        return [
            pltpu.make_async_copy(r1, w13b.at[at, :, pl.ds(0, ff)], a_sem.at[at, 0]),
            pltpu.make_async_copy(r3, w13b.at[at, :, pl.ds(ff, ff)], a_sem.at[at, 1]),
        ]

    def copies_b(r2, step):
        at = lax.rem(step, RING_B)
        return [pltpu.make_async_copy(r2, w2b.at[at], b_sem.at[at])]

    def expert_a(e):
        return copies_a(w1_hbm.at[e], w3_hbm.at[e], e + 1)

    def expert_b(e):
        return copies_b(w2_hbm.at[e], e + 1)

    def start_all(copies):
        for cp in copies:
            cp.start()

    shared_copies = copies_a(ws1_hbm, ws3_hbm, 0) + copies_b(ws2_hbm, 0)
    start_all(shared_copies)
    start_all(expert_a(0) + expert_b(0))

    barrier = pltpu.get_barrier_semaphore()
    for dev in ({"ep": part}, {"ep": far}, {"ep": far_part}, {"tp": 1 - tp}):
        pl.semaphore_signal(barrier, inc=1, device_id=dev, device_id_type=pl.DeviceIdType.MESH)

    for cp in small:
        cp.wait()
    eye = (lax.broadcasted_iota(jnp.int32, (n_exp, n_exp), 0)
           == lax.broadcasted_iota(jnp.int32, (n_exp, n_exp), 1))
    diag = jnp.where(eye, jnp.broadcast_to(cnt_v[...], (n_exp, n_exp)).astype(jnp.float32), 0.0)
    limit = dot(diag.astype(jnp.bfloat16), jnp.ones((n_exp, n_tok), jnp.bfloat16))
    g = gate_v[...]
    g1 = jnp.minimum(g, BF16_MAX).astype(jnp.bfloat16).astype(jnp.float32)
    g2 = (g - g1).astype(jnp.bfloat16).astype(jnp.float32)
    g3 = (g - g1) - g2
    slot_f = slot_v[...].astype(jnp.float32)
    ids = idx_v[...]
    row_e = lax.broadcasted_iota(jnp.int32, (n_exp, n_tok), 0)
    tabs = [jnp.zeros((n_exp, n_tok), jnp.float32) for _ in range(4)]
    for j in range(top_k):
        s_j = slot_f[j:j + 1, :]
        kept = (ids[j:j + 1, :] == row_e) & (s_j >= 0.0) & (s_j < limit)
        vals = (s_j + 1.0, g1[j:j + 1, :], g2[j:j + 1, :], g3[j:j + 1, :])
        tabs = [t + jnp.where(kept, v, 0.0) for t, v in zip(tabs, vals)]
    for q in range(n_src):
        for k in range(4):
            mt[q, k * n_local:(k + 1) * n_local, :] = (
                tabs[k][q * n_local:(q + 1) * n_local].astype(jnp.bfloat16))
    mr[ep] = mt[ep]

    pl.semaphore_wait(barrier, 4)

    def remote(src, dst, send, recv, dev):
        return pltpu.make_async_remote_copy(
            src_ref=src, dst_ref=dst, send_sem=send, recv_sem=recv,
            device_id=dev, device_id_type=pl.DeviceIdType.MESH)

    def one_copy(src, dst, k, dev):
        return remote(src, dst, send_sem.at[k], recv_sem.at[k], dev)

    def col_copies(src, dst, kind, dev):
        return [remote(src.at[:, pl.ds(c, w)], dst.at[:, pl.ds(c, w)],
                       col_send.at[kind, i], col_recv.at[kind, i], dev)
                for i, (c, w) in enumerate(cols)]

    m_far = one_copy(mt.at[far], mr.at[ep], M_FAR, {"ep": far})
    m_part = one_copy(mt.at[part], mr.at[ep], M_PART, {"ep": part})
    m_diag = one_copy(mt.at[far_part], mr.at[ep], M_DIAG, {"ep": far_part})
    x_far = col_copies(xs.at[ep], xs.at[ep], COL_X_FAR, {"ep": far})
    x_relay = col_copies(xs.at[far], xs.at[far], COL_X_RELAY, {"ep": part})
    x_y = one_copy(xs.at[ep], xy, X_Y, {"tp": 1 - tp})
    x_part = one_copy(xs.at[ep], xs.at[ep], X_PART, {"ep": part})
    m_far.start()
    m_diag.start()
    m_part.start()
    x_in.wait()
    start_all(x_far)
    x_part.start()
    x_y.start()

    for e in range(1, RING_A - 1):
        start_all(expert_a(e))
        if e < RING_B - 1:
            start_all(expert_b(e))

    def row_of(shape, dim):
        flat = lax.broadcasted_iota(jnp.int32, shape, dim)
        owner = lax.shift_right_logical(flat * 683, 15)
        return flat, owner

    def build_pick(s, i):
        _, owner = row_of((n_rows, 4 * n_local), 0)
        lanes = lax.broadcasted_iota(jnp.int32, (n_rows, 4 * n_local), 1)
        sel = jnp.where(lanes == owner, 1.0, 0.0).astype(jnp.bfloat16)
        at = dot(sel, mr[s])
        flat, owner = row_of((n_rows, n_tok), 0)
        want = (flat - owner * cap + 1).astype(jnp.float32)
        pk[i] = jnp.where(at == want, 1.0, 0.0).astype(jnp.bfloat16)

    def gather_cols(s, i, c, w):
        xr[s, :, c:c + w] = dot(pk[i], xs[s, :, c:c + w]).astype(jnp.bfloat16)

    def build_gates(s, i):
        tab = jnp.transpose(mr[s].astype(jnp.float32)).astype(jnp.bfloat16)
        lanes = lax.broadcasted_iota(jnp.int32, (4 * n_local, n_rows), 0)
        _, owner = row_of((4 * n_local, n_rows), 1)
        flat, own_t = row_of((n_tok, n_rows), 1)
        want = (flat - own_t * cap + 1).astype(jnp.float32)
        at = [dot(tab, jnp.where(lanes == owner + k * n_local, 1.0, 0.0).astype(jnp.bfloat16))
              for k in range(4)]
        hit = at[0] == want
        for k in range(3):
            gm[i, k] = jnp.where(hit, at[k + 1], 0.0).astype(jnp.bfloat16)

    def hidden(x_val, step, h_ref):
        rows = x_val.shape[0]
        slot = lax.rem(step, RING_A)
        for c, w in chunks(body):
            a = dot(x_val, w13b[slot, :, c:c + w])
            b = dot(x_val, w13b[slot, :, ff + c:ff + c + w])
            h_ref[0:rows, c:c + w] = (jax.nn.silu(a) * b).astype(jnp.bfloat16)
        ab = dot(x_val, jnp.concatenate([w13b[slot, :, body:ff], w13b[slot, :, ff + body:2 * ff]], axis=1))
        h_ref[0:rows, body:ff] = (jax.nn.silu(ab[:, 0:rest]) * ab[:, rest:2 * rest]).astype(jnp.bfloat16)

    def shared(x_val, out_ref):
        hidden(x_val, 0, hb.at[0])
        for c, w in cols:
            out_ref[:, c:c + w] = dot(hb[0, 0:n_tok, :], w2b[0, :, c:c + w])

    def wait_expert(e):
        for cp in expert_a(e) + expert_b(e):
            cp.wait()

    def refill(e):
        for copies, ring in ((expert_a, RING_A), (expert_b, RING_B)):
            @pl.when(e + ring < n_local)
            def _():
                start_all(copies(e + ring))

    def expert_slice(e):
        return pl.ds(pl.multiple_of(e * cap, 16), cap)

    def take_rows(e, sources):
        return jnp.concatenate([xr[s, expert_slice(e), :] for s in sources], axis=0)

    def expert_rows(e, sources, i):
        rows = expert_slice(e)
        n = len(sources) * cap
        hidden(take_rows(e, sources), e + 1, hb.at[i])
        for c, w in cols:
            out = dot(hb[i, 0:n, :], w2b[lax.rem(e + 1, RING_B), :, c:c + w]).astype(jnp.bfloat16)
            for k, s in enumerate(sources):
                xr[s, rows, c:c + w] = out[k * cap:(k + 1) * cap]

    build_pick(ep, 0)
    for c, w in cols:
        gather_cols(ep, 0, c, w)
    m_part.wait_recv()
    build_pick(part, 1)
    x_part.wait_recv()
    for c, w in cols:
        gather_cols(part, 1, c, w)
    for cp in shared_copies:
        cp.wait()
    shared(xs[ep], s_own)
    m_far.wait_recv()
    build_pick(far, 0)
    build_gates(far, 0)
    m_diag.wait_recv()
    build_pick(far_part, 1)
    build_gates(far_part, 1)
    build_gates(part, 2)
    build_gates(ep, 3)
    for e in range(NEAR):
        wait_expert(e)
    for e in range(NEAR):
        expert_rows(e, (ep, part), e % 2)

    for i, (c, w) in enumerate(cols):
        x_far[i].wait_recv()
        x_relay[i].start()
        gather_cols(far, 0, c, w)
    x_y.wait_recv()
    shared(xy[...], s_send)
    s_copy = one_copy(s_send, s_recv, S_Y, {"tp": 1 - tp})
    s_copy.start()
    start_all(expert_b(RING_B - 1) + expert_a(RING_A - 1))
    for i, (c, w) in enumerate(cols):
        x_relay[i].wait_recv()
        gather_cols(far_part, 1, c, w)
    for e in range(NEAR):
        expert_rows(e, (far, far_part), e % 2)
        start_all(expert_b(e + RING_B) + expert_a(e + RING_A))

    def pair_step(p, carry):
        both = [2 * p + i for i in range(2)]
        for e in both:
            wait_expert(e)
        for i, e in enumerate(both):
            expert_rows(e, range(n_src), i)
        for e in both:
            refill(e)

        return carry

    late = n_local - LAST
    lax.fori_loop(NEAR // 2, late // 2, pair_step, 0)

    def late_hidden(t, carry):
        both = [late + 2 * t + i for i in range(2)]
        for e in both:
            for cp in expert_a(e):
                cp.wait()
        for i, e in enumerate(both):
            hidden(take_rows(e, (far, far_part)), e + 1, hb.at[t, pl.ds(2 * i * cap, 2 * cap)])
        return carry

    lax.fori_loop(0, LAST // 2, late_hidden, 0)
    for e in range(late, n_local):
        for cp in expert_b(e):
            cp.wait()

    def combine(s, i, c, w):
        r = xr[s, :, c:c + w]
        return dot(gm[i, 0], r) + dot(gm[i, 1], r) + dot(gm[i, 2], r)

    a_copies = col_copies(a_send, a_recv, COL_A, {"ep": part})
    b_copies = col_copies(s_send, b_recv, COL_B, {"ep": far})
    s_copy.wait_send()

    def finish_b(i):
        c, w = cols[i]
        a_copies[i].wait_recv()
        s_send[:, c:c + w] += a_recv[:, c:c + w]
        b_copies[i].start()

    for i, (c, w) in enumerate(cols):
        for k, e in enumerate(range(late, n_local)):
            h = hb[k // 2, 2 * (k % 2) * cap:2 * (k % 2 + 1) * cap, :]
            out = dot(h, w2b[(e + 1) % RING_B, :, c:c + w]).astype(jnp.bfloat16)
            xr[far, e * cap:(e + 1) * cap, c:c + w] = out[0:cap]
            xr[far_part, e * cap:(e + 1) * cap, c:c + w] = out[cap:2 * cap]
        a_send[:, c:c + w] = combine(far_part, 1, c, w)
        a_copies[i].start()
        s_send[:, c:c + w] = combine(far, 0, c, w)
        if i > 0:
            finish_b(i - 1)
    finish_b(len(cols) - 1)
    pl.semaphore_signal(free_sem, inc=1, device_id={"ep": part}, device_id_type=pl.DeviceIdType.MESH)

    def late_near(t, carry):
        for i in range(2):
            e = late + 2 * t + i
            expert_rows(e, (ep, part), i)
        return carry

    lax.fori_loop(0, LAST // 2, late_near, 0)
    for cp in a_copies:
        cp.wait_send()
    for c, w in cols:
        a_send[:, c:c + w] = combine(part, 2, c, w)
    c_copy = one_copy(a_send, a_recv, C_PART, {"ep": part})
    pl.semaphore_wait(free_sem, 1)
    c_copy.start()
    for c, w in cols:
        s_own[:, c:c + w] += combine(ep, 3, c, w) + xs[ep, :, c:c + w].astype(jnp.float32)
    s_copy.wait_recv()
    c_copy.wait_recv()
    s_own[...] += s_recv[...] + a_recv[...]
    for i, (c, w) in enumerate(cols):
        b_copies[i].wait_recv()
        y_ref[:, c:c + w] = (s_own[:, c:c + w] + b_recv[:, c:c + w]).astype(jnp.bfloat16)

    for cp in [x_y, x_part, m_far, m_part, m_diag, c_copy] + x_far + x_relay + b_copies:
        cp.wait_send()


def solution(mesh):
    row_spec = P(("data", "ep", "tp"), None)
    expert_spec = P("ep", None, None)
    n_src = mesh.shape["ep"]

    def layer_body(tokens, expert_ids, gate_vals, slot_ids, send_counts, shared_w1, shared_w3, shared_w2, expert_w1, expert_w3, expert_w2):
        n_tok, d_model = tokens.shape
        top_k = expert_ids.shape[1]
        n_local, _, ff = expert_w1.shape
        n_exp = n_local * n_src
        cap = capacity_rows(n_tok, top_k, n_exp)
        n_rows = n_local * cap
        n_cols = len(chunks(d_model))
        block = pltpu.VMEM((n_tok, d_model), jnp.float32)
        local = [
                pltpu.VMEM((RING_A, d_model, 2 * ff), jnp.bfloat16),
                pltpu.VMEM((RING_B, ff, d_model), jnp.bfloat16),
                pltpu.VMEM((n_src, n_rows, d_model), jnp.bfloat16),
                pltpu.VMEM((LAST // 2, n_src * cap, ff), jnp.bfloat16),
                pltpu.VMEM((2, n_rows, n_tok), jnp.bfloat16),
                pltpu.VMEM((4, 3, n_tok, n_rows), jnp.bfloat16),
        ]

        def body(*refs):
            pl.run_scoped(functools.partial(kernel, cap, n_local, *refs), *local)

        return pl.pallas_call(
            body,
            out_shape=pltpu.VMEM((n_tok, d_model), jnp.bfloat16),
            in_specs=[pl.BlockSpec(memory_space=pl.ANY)] * 11,
            out_specs=pl.BlockSpec(memory_space=pltpu.VMEM),
            scratch_shapes=[
                pltpu.VMEM((n_src, n_tok, d_model), jnp.bfloat16),
                pltpu.VMEM((n_tok, d_model), jnp.bfloat16),
                pltpu.VMEM((top_k, n_tok), jnp.int32),
                pltpu.VMEM((top_k, n_tok), jnp.float32),
                pltpu.VMEM((top_k, n_tok), jnp.int32),
                pltpu.VMEM((1, n_exp), jnp.int32),
                pltpu.VMEM((n_src, 4 * n_local, n_tok), jnp.bfloat16),
                pltpu.VMEM((n_src, 4 * n_local, n_tok), jnp.bfloat16),
            ] + [block] * 6 + [
                pltpu.SemaphoreType.DMA((5,)),
                pltpu.SemaphoreType.DMA((RING_A, 2)),
                pltpu.SemaphoreType.DMA((RING_B,)),
                pltpu.SemaphoreType.DMA((N_COPIES,)),
                pltpu.SemaphoreType.DMA((N_COPIES,)),
                pltpu.SemaphoreType.DMA((N_COL_KINDS, n_cols)),
                pltpu.SemaphoreType.DMA((N_COL_KINDS, n_cols)),
                pltpu.SemaphoreType.REGULAR,
            ],
            compiler_params=pltpu.CompilerParams(
                collective_id=0, has_side_effects=True, vmem_limit_bytes=66500000),
            name="moe_layer",
        )(tokens, expert_ids.T, gate_vals.T, slot_ids.T, send_counts, shared_w1, shared_w3, shared_w2, expert_w1, expert_w3, expert_w2)

    return jax.shard_map(
        layer_body,
        mesh=mesh,
        in_specs=(row_spec, row_spec, row_spec, row_spec, row_spec, P(None, "tp"), P(None, "tp"), P("tp", None), expert_spec, expert_spec, expert_spec),
        out_specs=row_spec,
        check_vma=False,
    )
```

```python
import functools

import jax
import jax.numpy as jnp
from jax import lax
from jax.experimental import pallas as pl
from jax.experimental.pallas import tpu as pltpu
from jax.sharding import PartitionSpec as P

CAP_FACTOR = 4
BF16_MAX = 3.3895313892515355e38
RING_A = 7
RING_B = 6
NEAR = 2
LAST = 6

X_PART, X_Y, M_PART, M_FAR, M_DIAG, S_Y, C_PART = range(7)
N_COPIES = 7
COL_X_FAR, COL_X_RELAY, COL_A, COL_B = range(4)
N_COL_KINDS = 4


def capacity_rows(n_tok, top_k, n_exp):
    return min(n_tok, ((CAP_FACTOR * n_tok * top_k // n_exp + 7) // 8) * 8)


def chunks(n, step=256):
    return [(i, min(step, n - i)) for i in range(0, n, step)]


def dot(a, b):
    return jnp.dot(a, b, preferred_element_type=jnp.float32)


def dot_nt(a, b):
    return lax.dot_general(a, b, (((1,), (1,)), ((), ())), preferred_element_type=jnp.float32)


def kernel(cap, n_local,
           x_hbm, idx_hbm, gate_hbm, slot_hbm, cnt_hbm,
           ws1_hbm, ws3_hbm, ws2_hbm, w1_hbm, w3_hbm, w2_hbm,
           y_ref,
           xs, xy, idx_v, gate_v, slot_v, cnt_v, mt, mr,
           s_own, s_send, s_recv, a_send, a_recv, b_recv,
           in_sem, a_sem, b_sem, send_sem, recv_sem, col_send, col_recv, free_sem, w13b, w2b, xr, hb, pk, gm):
    n_tok, d_model = x_hbm.shape
    top_k = idx_hbm.shape[0]
    ff = w1_hbm.shape[2]
    body = ff // 256 * 256
    rest = ff - body
    n_src = xs.shape[0]
    n_exp = n_src * n_local
    n_rows = n_local * cap
    cols = chunks(d_model)

    ep = lax.axis_index("ep")
    tp = lax.axis_index("tp")
    part = ep + 1 - 2 * lax.rem(ep, 2)
    far = lax.rem(ep + 2, 4)
    far_part = lax.rem(part + 2, 4)

    x_in = pltpu.make_async_copy(x_hbm, xs.at[ep], in_sem.at[0])
    small = [
        pltpu.make_async_copy(idx_hbm, idx_v, in_sem.at[1]),
        pltpu.make_async_copy(gate_hbm, gate_v, in_sem.at[2]),
        pltpu.make_async_copy(slot_hbm, slot_v, in_sem.at[3]),
        pltpu.make_async_copy(cnt_hbm, cnt_v, in_sem.at[4]),
    ]
    for cp in small:
        cp.start()
    x_in.start()

    def copies_a(r1, r3, step):
        at = lax.rem(step, RING_A)
        return [
            pltpu.make_async_copy(r1, w13b.at[at, :, pl.ds(0, ff)], a_sem.at[at, 0]),
            pltpu.make_async_copy(r3, w13b.at[at, :, pl.ds(ff, ff)], a_sem.at[at, 1]),
        ]

    def copies_b(r2, step):
        at = lax.rem(step, RING_B)
        return [pltpu.make_async_copy(r2, w2b.at[at], b_sem.at[at])]

    def expert_a(e):
        return copies_a(w1_hbm.at[e], w3_hbm.at[e], e + 1)

    def expert_b(e):
        return copies_b(w2_hbm.at[e], e + 1)

    def start_all(copies):
        for cp in copies:
            cp.start()

    shared_copies = copies_a(ws1_hbm, ws3_hbm, 0) + copies_b(ws2_hbm, 0)
    start_all(shared_copies)
    start_all(expert_a(0) + expert_b(0))

    barrier = pltpu.get_barrier_semaphore()
    for dev in ({"ep": part}, {"ep": far}, {"ep": far_part}, {"tp": 1 - tp}):
        pl.semaphore_signal(barrier, inc=1, device_id=dev, device_id_type=pl.DeviceIdType.MESH)

    for cp in small:
        cp.wait()
    eye = (lax.broadcasted_iota(jnp.int32, (n_exp, n_exp), 0)
           == lax.broadcasted_iota(jnp.int32, (n_exp, n_exp), 1))
    diag = jnp.where(eye, jnp.broadcast_to(cnt_v[...], (n_exp, n_exp)).astype(jnp.float32), 0.0)
    limit = dot(diag.astype(jnp.bfloat16), jnp.ones((n_exp, n_tok), jnp.bfloat16))
    g = gate_v[...]
    g1 = jnp.minimum(g, BF16_MAX).astype(jnp.bfloat16).astype(jnp.float32)
    g2 = (g - g1).astype(jnp.bfloat16).astype(jnp.float32)
    g3 = (g - g1) - g2
    slot_f = slot_v[...].astype(jnp.float32)
    ids = idx_v[...]
    row_e = lax.broadcasted_iota(jnp.int32, (n_exp, n_tok), 0)
    tabs = [jnp.zeros((n_exp, n_tok), jnp.float32) for _ in range(4)]
    for j in range(top_k):
        s_j = slot_f[j:j + 1, :]
        kept = (ids[j:j + 1, :] == row_e) & (s_j >= 0.0) & (s_j < limit)
        vals = (s_j + 1.0, g1[j:j + 1, :], g2[j:j + 1, :], g3[j:j + 1, :])
        tabs = [t + jnp.where(kept, v, 0.0) for t, v in zip(tabs, vals)]
    for q in range(n_src):
        for k in range(4):
            mt[q, k * n_local:(k + 1) * n_local, :] = (
                tabs[k][q * n_local:(q + 1) * n_local].astype(jnp.bfloat16))
    mr[ep] = mt[ep]

    pl.semaphore_wait(barrier, 4)

    def remote(src, dst, send, recv, dev):
        return pltpu.make_async_remote_copy(
            src_ref=src, dst_ref=dst, send_sem=send, recv_sem=recv,
            device_id=dev, device_id_type=pl.DeviceIdType.MESH)

    def one_copy(src, dst, k, dev):
        return remote(src, dst, send_sem.at[k], recv_sem.at[k], dev)

    def col_copies(src, dst, kind, dev):
        return [remote(src.at[:, pl.ds(c, w)], dst.at[:, pl.ds(c, w)],
                       col_send.at[kind, i], col_recv.at[kind, i], dev)
                for i, (c, w) in enumerate(cols)]

    m_far = one_copy(mt.at[far], mr.at[ep], M_FAR, {"ep": far})
    m_part = one_copy(mt.at[part], mr.at[ep], M_PART, {"ep": part})
    m_diag = one_copy(mt.at[far_part], mr.at[ep], M_DIAG, {"ep": far_part})
    x_far = col_copies(xs.at[ep], xs.at[ep], COL_X_FAR, {"ep": far})
    x_relay = col_copies(xs.at[far], xs.at[far], COL_X_RELAY, {"ep": part})
    x_y = one_copy(xs.at[ep], xy, X_Y, {"tp": 1 - tp})
    x_part = one_copy(xs.at[ep], xs.at[ep], X_PART, {"ep": part})
    m_far.start()
    m_diag.start()
    m_part.start()
    x_in.wait()
    start_all(x_far)
    x_part.start()
    x_y.start()

    for e in range(1, RING_A - 1):
        start_all(expert_a(e))
        if e < RING_B - 1:
            start_all(expert_b(e))

    def row_of(shape, dim):
        flat = lax.broadcasted_iota(jnp.int32, shape, dim)
        owner = lax.shift_right_logical(flat * 683, 15)
        return flat, owner

    def build_pick(s, i):
        _, owner = row_of((n_rows, 4 * n_local), 0)
        lanes = lax.broadcasted_iota(jnp.int32, (n_rows, 4 * n_local), 1)
        sel = jnp.where(lanes == owner, 1.0, 0.0).astype(jnp.bfloat16)
        at = dot(sel, mr[s])
        flat, owner = row_of((n_rows, n_tok), 0)
        want = (flat - owner * cap + 1).astype(jnp.float32)
        pk[i] = jnp.where(at == want, 1.0, 0.0).astype(jnp.bfloat16)

    def gather_cols(s, i, c, w):
        xr[s, :, c:c + w] = dot(pk[i], xs[s, :, c:c + w]).astype(jnp.bfloat16)

    def build_gates(s, i):
        tab = jnp.transpose(mr[s].astype(jnp.float32)).astype(jnp.bfloat16)
        lanes = lax.broadcasted_iota(jnp.int32, (4 * n_local, n_rows), 0)
        _, owner = row_of((4 * n_local, n_rows), 1)
        flat, own_t = row_of((n_tok, n_rows), 1)
        want = (flat - own_t * cap + 1).astype(jnp.float32)
        at = [dot(tab, jnp.where(lanes == owner + k * n_local, 1.0, 0.0).astype(jnp.bfloat16))
              for k in range(4)]
        hit = at[0] == want
        for k in range(3):
            gm[i, k] = jnp.where(hit, at[k + 1], 0.0).astype(jnp.bfloat16)

    def hidden(x_val, step, h_ref):
        rows = x_val.shape[0]
        slot = lax.rem(step, RING_A)
        for c, w in chunks(body):
            a = dot(x_val, w13b[slot, :, c:c + w])
            b = dot(x_val, w13b[slot, :, ff + c:ff + c + w])
            h_ref[0:rows, c:c + w] = (jax.nn.silu(a) * b).astype(jnp.bfloat16)
        ab = dot(x_val, jnp.concatenate([w13b[slot, :, body:ff], w13b[slot, :, ff + body:2 * ff]], axis=1))
        h_ref[0:rows, body:ff] = (jax.nn.silu(ab[:, 0:rest]) * ab[:, rest:2 * rest]).astype(jnp.bfloat16)

    def shared(x_val, out_ref):
        hidden(x_val, 0, hb.at[0])
        for c, w in cols:
            out_ref[:, c:c + w] = dot(hb[0, 0:n_tok, :], w2b[0, :, c:c + w])

    def wait_expert(e):
        for cp in expert_a(e) + expert_b(e):
            cp.wait()

    def refill(e):
        for copies, ring in ((expert_a, RING_A), (expert_b, RING_B)):
            @pl.when(e + ring < n_local)
            def _():
                start_all(copies(e + ring))

    def expert_slice(e):
        return pl.ds(pl.multiple_of(e * cap, 16), cap)

    def take_rows(e, sources):
        return jnp.concatenate([xr[s, expert_slice(e), :] for s in sources], axis=0)

    def expert_rows(e, sources, i):
        rows = expert_slice(e)
        n = len(sources) * cap
        hidden(take_rows(e, sources), e + 1, hb.at[i])
        for c, w in cols:
            out = dot(hb[i, 0:n, :], w2b[lax.rem(e + 1, RING_B), :, c:c + w]).astype(jnp.bfloat16)
            for k, s in enumerate(sources):
                xr[s, rows, c:c + w] = out[k * cap:(k + 1) * cap]

    build_pick(ep, 0)
    for c, w in cols:
        gather_cols(ep, 0, c, w)
    m_part.wait_recv()
    build_pick(part, 1)
    x_part.wait_recv()
    for c, w in cols:
        gather_cols(part, 1, c, w)
    for cp in shared_copies:
        cp.wait()
    shared(xs[ep], s_own)
    m_far.wait_recv()
    build_pick(far, 0)
    build_gates(far, 0)
    m_diag.wait_recv()
    build_pick(far_part, 1)
    build_gates(far_part, 1)
    build_gates(part, 2)
    build_gates(ep, 3)
    for e in range(NEAR):
        wait_expert(e)
    for e in range(NEAR):
        expert_rows(e, (ep, part), e % 2)

    for i, (c, w) in enumerate(cols):
        x_far[i].wait_recv()
        x_relay[i].start()
        gather_cols(far, 0, c, w)
    x_y.wait_recv()
    shared(xy[...], s_send)
    s_copy = one_copy(s_send, s_recv, S_Y, {"tp": 1 - tp})
    s_copy.start()
    start_all(expert_b(RING_B - 1) + expert_a(RING_A - 1))
    for i, (c, w) in enumerate(cols):
        x_relay[i].wait_recv()
        gather_cols(far_part, 1, c, w)
    for e in range(NEAR):
        expert_rows(e, (far, far_part), e % 2)
        start_all(expert_b(e + RING_B) + expert_a(e + RING_A))

    def pair_step(p, carry):
        both = [2 * p + i for i in range(2)]
        for e in both:
            wait_expert(e)
        for i, e in enumerate(both):
            expert_rows(e, range(n_src), i)
        for e in both:
            refill(e)

        return carry

    late = n_local - LAST
    lax.fori_loop(NEAR // 2, late // 2, pair_step, 0)

    def late_hidden(t, carry):
        both = [late + 2 * t + i for i in range(2)]
        for e in both:
            for cp in expert_a(e):
                cp.wait()
        for i, e in enumerate(both):
            hidden(take_rows(e, (far, far_part)), e + 1, hb.at[t, pl.ds(2 * i * cap, 2 * cap)])
        return carry

    lax.fori_loop(0, LAST // 2, late_hidden, 0)
    for e in range(late, n_local):
        for cp in expert_b(e):
            cp.wait()

    def combine(s, i, c, w):
        r = xr[s, :, c:c + w]
        return dot(gm[i, 0], r) + dot(gm[i, 1], r) + dot(gm[i, 2], r)

    a_copies = col_copies(a_send, a_recv, COL_A, {"ep": part})
    b_copies = col_copies(s_send, b_recv, COL_B, {"ep": far})
    s_copy.wait_send()

    def finish_b(i):
        c, w = cols[i]
        a_copies[i].wait_recv()
        s_send[:, c:c + w] += a_recv[:, c:c + w]
        b_copies[i].start()

    for i, (c, w) in enumerate(cols):
        for k, e in enumerate(range(late, n_local)):
            h = hb[k // 2, 2 * (k % 2) * cap:2 * (k % 2 + 1) * cap, :]
            out = dot(h, w2b[(e + 1) % RING_B, :, c:c + w]).astype(jnp.bfloat16)
            xr[far, e * cap:(e + 1) * cap, c:c + w] = out[0:cap]
            xr[far_part, e * cap:(e + 1) * cap, c:c + w] = out[cap:2 * cap]
        a_send[:, c:c + w] = combine(far_part, 1, c, w)
        a_copies[i].start()
        if i > 0:
            finish_b(i - 1)
        s_send[:, c:c + w] = combine(far, 0, c, w)
    finish_b(len(cols) - 1)
    pl.semaphore_signal(free_sem, inc=1, device_id={"ep": part}, device_id_type=pl.DeviceIdType.MESH)

    def late_near(t, carry):
        for i in range(2):
            e = late + 2 * t + i
            expert_rows(e, (ep, part), i)
        return carry

    lax.fori_loop(0, LAST // 2, late_near, 0)
    for cp in a_copies:
        cp.wait_send()
    for c, w in cols:
        a_send[:, c:c + w] = combine(part, 2, c, w)
    c_copy = one_copy(a_send, a_recv, C_PART, {"ep": part})
    pl.semaphore_wait(free_sem, 1)
    c_copy.start()
    for c, w in cols:
        s_own[:, c:c + w] += combine(ep, 3, c, w) + xs[ep, :, c:c + w].astype(jnp.float32)
    s_copy.wait_recv()
    c_copy.wait_recv()
    s_own[...] += s_recv[...] + a_recv[...]
    for i, (c, w) in enumerate(cols):
        b_copies[i].wait_recv()
        y_ref[:, c:c + w] = (s_own[:, c:c + w] + b_recv[:, c:c + w]).astype(jnp.bfloat16)

    for cp in [x_y, x_part, m_far, m_part, m_diag, c_copy] + x_far + x_relay + b_copies:
        cp.wait_send()


def solution(mesh):
    row_spec = P(("data", "ep", "tp"), None)
    expert_spec = P("ep", None, None)
    n_src = mesh.shape["ep"]

    def layer_body(tokens, expert_ids, gate_vals, slot_ids, send_counts, shared_w1, shared_w3, shared_w2, expert_w1, expert_w3, expert_w2):
        n_tok, d_model = tokens.shape
        top_k = expert_ids.shape[1]
        n_local, _, ff = expert_w1.shape
        n_exp = n_local * n_src
        cap = capacity_rows(n_tok, top_k, n_exp)
        n_rows = n_local * cap
        n_cols = len(chunks(d_model))
        block = pltpu.VMEM((n_tok, d_model), jnp.float32)
        local = [
                pltpu.VMEM((RING_A, d_model, 2 * ff), jnp.bfloat16),
                pltpu.VMEM((RING_B, ff, d_model), jnp.bfloat16),
                pltpu.VMEM((n_src, n_rows, d_model), jnp.bfloat16),
                pltpu.VMEM((LAST // 2, n_src * cap, ff), jnp.bfloat16),
                pltpu.VMEM((2, n_rows, n_tok), jnp.bfloat16),
                pltpu.VMEM((4, 3, n_tok, n_rows), jnp.bfloat16),
        ]

        def body(*refs):
            pl.run_scoped(functools.partial(kernel, cap, n_local, *refs), *local)

        return pl.pallas_call(
            body,
            out_shape=pltpu.VMEM((n_tok, d_model), jnp.bfloat16),
            in_specs=[pl.BlockSpec(memory_space=pl.ANY)] * 11,
            out_specs=pl.BlockSpec(memory_space=pltpu.VMEM),
            scratch_shapes=[
                pltpu.VMEM((n_src, n_tok, d_model), jnp.bfloat16),
                pltpu.VMEM((n_tok, d_model), jnp.bfloat16),
                pltpu.VMEM((top_k, n_tok), jnp.int32),
                pltpu.VMEM((top_k, n_tok), jnp.float32),
                pltpu.VMEM((top_k, n_tok), jnp.int32),
                pltpu.VMEM((1, n_exp), jnp.int32),
                pltpu.VMEM((n_src, 4 * n_local, n_tok), jnp.bfloat16),
                pltpu.VMEM((n_src, 4 * n_local, n_tok), jnp.bfloat16),
            ] + [block] * 6 + [
                pltpu.SemaphoreType.DMA((5,)),
                pltpu.SemaphoreType.DMA((RING_A, 2)),
                pltpu.SemaphoreType.DMA((RING_B,)),
                pltpu.SemaphoreType.DMA((N_COPIES,)),
                pltpu.SemaphoreType.DMA((N_COPIES,)),
                pltpu.SemaphoreType.DMA((N_COL_KINDS, n_cols)),
                pltpu.SemaphoreType.DMA((N_COL_KINDS, n_cols)),
                pltpu.SemaphoreType.REGULAR,
            ],
            compiler_params=pltpu.CompilerParams(
                collective_id=0, has_side_effects=True, vmem_limit_bytes=66500000),
            name="moe_layer",
        )(tokens, expert_ids.T, gate_vals.T, slot_ids.T, send_counts, shared_w1, shared_w3, shared_w2, expert_w1, expert_w3, expert_w2)

    return jax.shard_map(
        layer_body,
        mesh=mesh,
        in_specs=(row_spec, row_spec, row_spec, row_spec, row_spec, P(None, "tp"), P(None, "tp"), P("tp", None), expert_spec, expert_spec, expert_spec),
        out_specs=row_spec,
        check_vma=False,
    )
```

```python
import functools

import jax
import jax.numpy as jnp
from jax import lax
from jax.experimental import pallas as pl
from jax.experimental.pallas import tpu as pltpu
from jax.sharding import PartitionSpec as P

CAP_FACTOR = 4
BF16_MAX = 3.3895313892515355e38
RING_A = 7
RING_B = 6
NEAR = 2
LAST = 6

X_PART, X_Y, M_PART, M_FAR, M_DIAG, S_Y = range(6)
N_COPIES = 6
COL_X_FAR, COL_X_RELAY, COL_A, COL_B, COL_C = range(5)
N_COL_KINDS = 5


def capacity_rows(n_tok, top_k, n_exp):
    return min(n_tok, ((CAP_FACTOR * n_tok * top_k // n_exp + 7) // 8) * 8)


def chunks(n, step=256):
    return [(i, min(step, n - i)) for i in range(0, n, step)]


def dot(a, b):
    return jnp.dot(a, b, preferred_element_type=jnp.float32)


def dot_nt(a, b):
    return lax.dot_general(a, b, (((1,), (1,)), ((), ())), preferred_element_type=jnp.float32)


def kernel(cap, n_local,
           x_hbm, idx_hbm, gate_hbm, slot_hbm, cnt_hbm,
           ws1_hbm, ws3_hbm, ws2_hbm, w1_hbm, w3_hbm, w2_hbm,
           y_ref,
           xs, xy, idx_v, gate_v, slot_v, cnt_v, mt, mr,
           s_own, s_send, s_recv, a_send, a_recv, b_recv,
           in_sem, a_sem, b_sem, send_sem, recv_sem, col_send, col_recv, free_sem, w13b, w2b, xr, hb, pk, gm):
    n_tok, d_model = x_hbm.shape
    top_k = idx_hbm.shape[0]
    ff = w1_hbm.shape[2]
    body = ff // 256 * 256
    rest = ff - body
    n_src = xs.shape[0]
    n_exp = n_src * n_local
    n_rows = n_local * cap
    cols = chunks(d_model)

    ep = lax.axis_index("ep")
    tp = lax.axis_index("tp")
    part = ep + 1 - 2 * lax.rem(ep, 2)
    far = lax.rem(ep + 2, 4)
    far_part = lax.rem(part + 2, 4)

    x_in = pltpu.make_async_copy(x_hbm, xs.at[ep], in_sem.at[0])
    small = [
        pltpu.make_async_copy(idx_hbm, idx_v, in_sem.at[1]),
        pltpu.make_async_copy(gate_hbm, gate_v, in_sem.at[2]),
        pltpu.make_async_copy(slot_hbm, slot_v, in_sem.at[3]),
        pltpu.make_async_copy(cnt_hbm, cnt_v, in_sem.at[4]),
    ]
    for cp in small:
        cp.start()
    x_in.start()

    def copies_a(r1, r3, step):
        at = lax.rem(step, RING_A)
        return [
            pltpu.make_async_copy(r1, w13b.at[at, :, pl.ds(0, ff)], a_sem.at[at, 0]),
            pltpu.make_async_copy(r3, w13b.at[at, :, pl.ds(ff, ff)], a_sem.at[at, 1]),
        ]

    def copies_b(r2, step):
        at = lax.rem(step, RING_B)
        return [pltpu.make_async_copy(r2, w2b.at[at], b_sem.at[at])]

    def expert_a(e):
        return copies_a(w1_hbm.at[e], w3_hbm.at[e], e + 1)

    def expert_b(e):
        return copies_b(w2_hbm.at[e], e + 1)

    def start_all(copies):
        for cp in copies:
            cp.start()

    shared_copies = copies_a(ws1_hbm, ws3_hbm, 0) + copies_b(ws2_hbm, 0)
    start_all(shared_copies)
    start_all(expert_a(0) + expert_b(0))

    barrier = pltpu.get_barrier_semaphore()
    for dev in ({"ep": part}, {"ep": far}, {"ep": far_part}, {"tp": 1 - tp}):
        pl.semaphore_signal(barrier, inc=1, device_id=dev, device_id_type=pl.DeviceIdType.MESH)

    for cp in small:
        cp.wait()
    eye = (lax.broadcasted_iota(jnp.int32, (n_exp, n_exp), 0)
           == lax.broadcasted_iota(jnp.int32, (n_exp, n_exp), 1))
    diag = jnp.where(eye, jnp.broadcast_to(cnt_v[...], (n_exp, n_exp)).astype(jnp.float32), 0.0)
    limit = dot(diag.astype(jnp.bfloat16), jnp.ones((n_exp, n_tok), jnp.bfloat16))
    g = gate_v[...]
    g1 = jnp.minimum(g, BF16_MAX).astype(jnp.bfloat16).astype(jnp.float32)
    g2 = (g - g1).astype(jnp.bfloat16).astype(jnp.float32)
    g3 = (g - g1) - g2
    slot_f = slot_v[...].astype(jnp.float32)
    ids = idx_v[...]
    row_e = lax.broadcasted_iota(jnp.int32, (n_exp, n_tok), 0)
    tabs = [jnp.zeros((n_exp, n_tok), jnp.float32) for _ in range(4)]
    for j in range(top_k):
        s_j = slot_f[j:j + 1, :]
        kept = (ids[j:j + 1, :] == row_e) & (s_j >= 0.0) & (s_j < limit)
        vals = (s_j + 1.0, g1[j:j + 1, :], g2[j:j + 1, :], g3[j:j + 1, :])
        tabs = [t + jnp.where(kept, v, 0.0) for t, v in zip(tabs, vals)]
    for q in range(n_src):
        for k in range(4):
            mt[q, k * n_local:(k + 1) * n_local, :] = (
                tabs[k][q * n_local:(q + 1) * n_local].astype(jnp.bfloat16))
    mr[ep] = mt[ep]

    pl.semaphore_wait(barrier, 4)

    def remote(src, dst, send, recv, dev):
        return pltpu.make_async_remote_copy(
            src_ref=src, dst_ref=dst, send_sem=send, recv_sem=recv,
            device_id=dev, device_id_type=pl.DeviceIdType.MESH)

    def one_copy(src, dst, k, dev):
        return remote(src, dst, send_sem.at[k], recv_sem.at[k], dev)

    def col_copies(src, dst, kind, dev):
        return [remote(src.at[:, pl.ds(c, w)], dst.at[:, pl.ds(c, w)],
                       col_send.at[kind, i], col_recv.at[kind, i], dev)
                for i, (c, w) in enumerate(cols)]

    m_far = one_copy(mt.at[far], mr.at[ep], M_FAR, {"ep": far})
    m_part = one_copy(mt.at[part], mr.at[ep], M_PART, {"ep": part})
    m_diag = one_copy(mt.at[far_part], mr.at[ep], M_DIAG, {"ep": far_part})
    x_far = col_copies(xs.at[ep], xs.at[ep], COL_X_FAR, {"ep": far})
    x_relay = col_copies(xs.at[far], xs.at[far], COL_X_RELAY, {"ep": part})
    x_y = one_copy(xs.at[ep], xy, X_Y, {"tp": 1 - tp})
    x_part = one_copy(xs.at[ep], xs.at[ep], X_PART, {"ep": part})
    m_far.start()
    m_diag.start()
    m_part.start()
    x_in.wait()
    start_all(x_far)
    x_part.start()
    x_y.start()

    for e in range(1, RING_A - 1):
        start_all(expert_a(e))
        if e < RING_B - 1:
            start_all(expert_b(e))

    def row_of(shape, dim):
        flat = lax.broadcasted_iota(jnp.int32, shape, dim)
        owner = lax.shift_right_logical(flat * 683, 15)
        return flat, owner

    def build_pick(s, i):
        _, owner = row_of((n_rows, 4 * n_local), 0)
        lanes = lax.broadcasted_iota(jnp.int32, (n_rows, 4 * n_local), 1)
        sel = jnp.where(lanes == owner, 1.0, 0.0).astype(jnp.bfloat16)
        at = dot(sel, mr[s])
        flat, owner = row_of((n_rows, n_tok), 0)
        want = (flat - owner * cap + 1).astype(jnp.float32)
        pk[i] = jnp.where(at == want, 1.0, 0.0).astype(jnp.bfloat16)

    def gather_cols(s, i, c, w):
        xr[s, :, c:c + w] = dot(pk[i], xs[s, :, c:c + w]).astype(jnp.bfloat16)

    def build_gates(s, i):
        tab = jnp.transpose(mr[s].astype(jnp.float32)).astype(jnp.bfloat16)
        lanes = lax.broadcasted_iota(jnp.int32, (4 * n_local, n_rows), 0)
        _, owner = row_of((4 * n_local, n_rows), 1)
        flat, own_t = row_of((n_tok, n_rows), 1)
        want = (flat - own_t * cap + 1).astype(jnp.float32)
        at = [dot(tab, jnp.where(lanes == owner + k * n_local, 1.0, 0.0).astype(jnp.bfloat16))
              for k in range(4)]
        hit = at[0] == want
        for k in range(3):
            gm[i, k] = jnp.where(hit, at[k + 1], 0.0).astype(jnp.bfloat16)

    def hidden(x_val, step, h_ref):
        rows = x_val.shape[0]
        slot = lax.rem(step, RING_A)
        for c, w in chunks(body):
            a = dot(x_val, w13b[slot, :, c:c + w])
            b = dot(x_val, w13b[slot, :, ff + c:ff + c + w])
            h_ref[0:rows, c:c + w] = (jax.nn.silu(a) * b).astype(jnp.bfloat16)
        ab = dot(x_val, jnp.concatenate([w13b[slot, :, body:ff], w13b[slot, :, ff + body:2 * ff]], axis=1))
        h_ref[0:rows, body:ff] = (jax.nn.silu(ab[:, 0:rest]) * ab[:, rest:2 * rest]).astype(jnp.bfloat16)

    def shared(x_val, out_ref):
        hidden(x_val, 0, hb.at[0])
        for c, w in cols:
            out_ref[:, c:c + w] = dot(hb[0, 0:n_tok, :], w2b[0, :, c:c + w])

    def wait_expert(e):
        for cp in expert_a(e) + expert_b(e):
            cp.wait()

    def refill(e):
        for copies, ring in ((expert_a, RING_A), (expert_b, RING_B)):
            @pl.when(e + ring < n_local)
            def _():
                start_all(copies(e + ring))

    def expert_slice(e):
        return pl.ds(pl.multiple_of(e * cap, 16), cap)

    def take_rows(e, sources):
        return jnp.concatenate([xr[s, expert_slice(e), :] for s in sources], axis=0)

    def expert_rows(e, sources, i):
        rows = expert_slice(e)
        n = len(sources) * cap
        hidden(take_rows(e, sources), e + 1, hb.at[i])
        for c, w in cols:
            out = dot(hb[i, 0:n, :], w2b[lax.rem(e + 1, RING_B), :, c:c + w]).astype(jnp.bfloat16)
            for k, s in enumerate(sources):
                xr[s, rows, c:c + w] = out[k * cap:(k + 1) * cap]

    build_pick(ep, 0)
    for c, w in cols:
        gather_cols(ep, 0, c, w)
    m_part.wait_recv()
    build_pick(part, 1)
    x_part.wait_recv()
    for c, w in cols:
        gather_cols(part, 1, c, w)
    for cp in shared_copies:
        cp.wait()
    shared(xs[ep], s_own)
    m_far.wait_recv()
    build_pick(far, 0)
    build_gates(far, 0)
    m_diag.wait_recv()
    build_pick(far_part, 1)
    build_gates(far_part, 1)
    build_gates(part, 2)
    build_gates(ep, 3)
    for e in range(NEAR):
        wait_expert(e)
    for e in range(NEAR):
        expert_rows(e, (ep, part), e % 2)

    for i, (c, w) in enumerate(cols):
        x_far[i].wait_recv()
        x_relay[i].start()
        gather_cols(far, 0, c, w)
    x_y.wait_recv()
    shared(xy[...], s_send)
    s_copy = one_copy(s_send, s_recv, S_Y, {"tp": 1 - tp})
    s_copy.start()
    start_all(expert_b(RING_B - 1) + expert_a(RING_A - 1))
    for i, (c, w) in enumerate(cols):
        x_relay[i].wait_recv()
        gather_cols(far_part, 1, c, w)
    for e in range(NEAR):
        expert_rows(e, (far, far_part), e % 2)
        start_all(expert_b(e + RING_B) + expert_a(e + RING_A))

    def pair_step(p, carry):
        both = [2 * p + i for i in range(2)]
        for e in both:
            wait_expert(e)
        for i, e in enumerate(both):
            expert_rows(e, range(n_src), i)
        for e in both:
            refill(e)

        return carry

    late = n_local - LAST
    lax.fori_loop(NEAR // 2, late // 2, pair_step, 0)

    def late_hidden(t, carry):
        both = [late + 2 * t + i for i in range(2)]
        for e in both:
            for cp in expert_a(e):
                cp.wait()
        for i, e in enumerate(both):
            hidden(take_rows(e, (far, far_part)), e + 1, hb.at[t, pl.ds(2 * i * cap, 2 * cap)])
        return carry

    lax.fori_loop(0, LAST // 2, late_hidden, 0)
    for e in range(late, n_local):
        for cp in expert_b(e):
            cp.wait()

    def combine(s, i, c, w):
        r = xr[s, :, c:c + w]
        return dot(gm[i, 0], r) + dot(gm[i, 1], r) + dot(gm[i, 2], r)

    a_copies = col_copies(a_send, a_recv, COL_A, {"ep": part})
    b_copies = col_copies(s_send, b_recv, COL_B, {"ep": far})
    s_copy.wait_send()

    def finish_b(i):
        c, w = cols[i]
        a_copies[i].wait_recv()
        s_send[:, c:c + w] += a_recv[:, c:c + w]
        b_copies[i].start()

    for i, (c, w) in enumerate(cols):
        for k, e in enumerate(range(late, n_local)):
            h = hb[k // 2, 2 * (k % 2) * cap:2 * (k % 2 + 1) * cap, :]
            out = dot(h, w2b[(e + 1) % RING_B, :, c:c + w]).astype(jnp.bfloat16)
            xr[far, e * cap:(e + 1) * cap, c:c + w] = out[0:cap]
            xr[far_part, e * cap:(e + 1) * cap, c:c + w] = out[cap:2 * cap]
        a_send[:, c:c + w] = combine(far_part, 1, c, w)
        a_copies[i].start()
        if i > 0:
            finish_b(i - 1)
        s_send[:, c:c + w] = combine(far, 0, c, w)
    finish_b(len(cols) - 1)
    pl.semaphore_signal(free_sem, inc=1, device_id={"ep": part}, device_id_type=pl.DeviceIdType.MESH)

    def late_near(t, carry):
        for i in range(2):
            e = late + 2 * t + i
            expert_rows(e, (ep, part), i)
        return carry

    lax.fori_loop(0, LAST // 2, late_near, 0)
    for cp in a_copies:
        cp.wait_send()
    c_copies = col_copies(a_send, a_recv, COL_C, {"ep": part})
    pl.semaphore_wait(free_sem, 1)
    for i, (c, w) in enumerate(cols):
        a_send[:, c:c + w] = combine(part, 2, c, w)
        c_copies[i].start()
    s_copy.wait_recv()
    for c, w in cols:
        s_own[:, c:c + w] += (combine(ep, 3, c, w) + xs[ep, :, c:c + w].astype(jnp.float32)
                              + s_recv[:, c:c + w])
    for i, (c, w) in enumerate(cols):
        c_copies[i].wait_recv()
        s_own[:, c:c + w] += a_recv[:, c:c + w]
    for i, (c, w) in enumerate(cols):
        b_copies[i].wait_recv()
        y_ref[:, c:c + w] = (s_own[:, c:c + w] + b_recv[:, c:c + w]).astype(jnp.bfloat16)

    for cp in [x_y, x_part, m_far, m_part, m_diag] + x_far + x_relay + b_copies + c_copies:
        cp.wait_send()


def solution(mesh):
    row_spec = P(("data", "ep", "tp"), None)
    expert_spec = P("ep", None, None)
    n_src = mesh.shape["ep"]

    def layer_body(tokens, expert_ids, gate_vals, slot_ids, send_counts, shared_w1, shared_w3, shared_w2, expert_w1, expert_w3, expert_w2):
        n_tok, d_model = tokens.shape
        top_k = expert_ids.shape[1]
        n_local, _, ff = expert_w1.shape
        n_exp = n_local * n_src
        cap = capacity_rows(n_tok, top_k, n_exp)
        n_rows = n_local * cap
        n_cols = len(chunks(d_model))
        block = pltpu.VMEM((n_tok, d_model), jnp.float32)
        local = [
                pltpu.VMEM((RING_A, d_model, 2 * ff), jnp.bfloat16),
                pltpu.VMEM((RING_B, ff, d_model), jnp.bfloat16),
                pltpu.VMEM((n_src, n_rows, d_model), jnp.bfloat16),
                pltpu.VMEM((LAST // 2, n_src * cap, ff), jnp.bfloat16),
                pltpu.VMEM((2, n_rows, n_tok), jnp.bfloat16),
                pltpu.VMEM((4, 3, n_tok, n_rows), jnp.bfloat16),
        ]

        def body(*refs):
            pl.run_scoped(functools.partial(kernel, cap, n_local, *refs), *local)

        return pl.pallas_call(
            body,
            out_shape=pltpu.VMEM((n_tok, d_model), jnp.bfloat16),
            in_specs=[pl.BlockSpec(memory_space=pl.ANY)] * 11,
            out_specs=pl.BlockSpec(memory_space=pltpu.VMEM),
            scratch_shapes=[
                pltpu.VMEM((n_src, n_tok, d_model), jnp.bfloat16),
                pltpu.VMEM((n_tok, d_model), jnp.bfloat16),
                pltpu.VMEM((top_k, n_tok), jnp.int32),
                pltpu.VMEM((top_k, n_tok), jnp.float32),
                pltpu.VMEM((top_k, n_tok), jnp.int32),
                pltpu.VMEM((1, n_exp), jnp.int32),
                pltpu.VMEM((n_src, 4 * n_local, n_tok), jnp.bfloat16),
                pltpu.VMEM((n_src, 4 * n_local, n_tok), jnp.bfloat16),
            ] + [block] * 6 + [
                pltpu.SemaphoreType.DMA((5,)),
                pltpu.SemaphoreType.DMA((RING_A, 2)),
                pltpu.SemaphoreType.DMA((RING_B,)),
                pltpu.SemaphoreType.DMA((N_COPIES,)),
                pltpu.SemaphoreType.DMA((N_COPIES,)),
                pltpu.SemaphoreType.DMA((N_COL_KINDS, n_cols)),
                pltpu.SemaphoreType.DMA((N_COL_KINDS, n_cols)),
                pltpu.SemaphoreType.REGULAR,
            ],
            compiler_params=pltpu.CompilerParams(
                collective_id=0, has_side_effects=True, vmem_limit_bytes=66500000),
            name="moe_layer",
        )(tokens, expert_ids.T, gate_vals.T, slot_ids.T, send_counts, shared_w1, shared_w3, shared_w2, expert_w1, expert_w3, expert_w2)

    return jax.shard_map(
        layer_body,
        mesh=mesh,
        in_specs=(row_spec, row_spec, row_spec, row_spec, row_spec, P(None, "tp"), P(None, "tp"), P("tp", None), expert_spec, expert_spec, expert_spec),
        out_specs=row_spec,
        check_vma=False,
    )
```
